256 devices in a mesh: tm: 8 (over z_hi, x), space: 32 (over y, z_lo, core).
Axes of the slice: x: 4, y: 4, z: 8 (z_hi: 2, z_lo: 4; z = z_hi * 4 + z_lo), core: 2. Of those that a mesh axis runs over, the one named last changes fastest.
Arguments:
- increment: float32 [16, 5, 48, 256, 128], P('tm', None, None, 'space'), may hold values from -6 to 6
- multiplier: float32 [16, 5, 48, 256, 128], P('tm', None, None, 'space'), may hold values from -20 to 20
- sensor_multiplier: float32 [16, 2048], P('tm'), may hold values from -6 to 6
- misfit: float32 [16, 5, 48, 256, 128], P('tm', None, None, 'space'), may hold values from -20 to 20
- innovation: float32 [16, 2048], P('tm'), may hold values from -6 to 6
- model_error: float32 [5, 48], replicated, may hold values from 0.2 to 1
- sensor_error: float32 [16, 2048], P('tm'), may hold values from 0.3 to 1.5
- trajectory: bfloat16 [16, 2, 2, 48, 256, 128], P('tm', None, None, None, 'space'), may hold values from 0 to 1
- land_sea: int32 [256, 128], P('space'), may hold values 0 or 1
- sensor_cells: int32 [16, 2048], P('tm'), may hold values from 0 to 3145727
Outputs:
- increment_next: float32 [16, 5, 48, 256, 128], P('tm', None, None, 'space')
- multiplier_next: float32 [16, 5, 48, 256, 128], P('tm', None, None, 'space')
- sensor_next: float32 [16, 2048], P('tm')
The draws below stay inside these ranges and needn't reach their ends.
Inputs may be any that keep to these rules, and one draw needn't show every extreme that they name: `sensor_cells`: the flat index ((f * 48 + l) * 256 + x) * 128 + y of the observed cell at field f (0 temperature, 1 salinity), level l, column x, row y; an index may repeat.
All inputs are finite; a program needn't handle non-finite values. No bound on the sum of `land_sea` on one device may be relied on, other than what follows from the above.
Results may differ from the reference program's by a relative error of at most 0.0017.
Values may be sent and summed in bfloat16 or wider, within the bound.
A program may use at most 64 MiB of HBM per device.

```python
import math
import jax
import jax.numpy as jnp
from jax import lax

NY = 128
LEV = 48
STEPS = 2
NOBS = 2048
SUBWINDOWS = 16
NX = 256


def ramped_field(key, salt_code):
    local_key = jax.random.fold_in(key, salt_code)
    shape = (SUBWINDOWS, 5, LEV, NX, NY)
    timing = jnp.arange(SUBWINDOWS, dtype=jnp.float32) / max(SUBWINDOWS - 1, 1)
    longitude = jnp.arange(NX, dtype=jnp.float32) / max(NX - 1, 1)
    base = jax.random.truncated_normal(local_key, -6.0, 6.0, shape, jnp.float32)
    exponent = 0.5 * timing[:, None, None, None, None] + 0.5 * longitude[None, None, None, :, None]
    return base * 10.0 ** exponent / 3.0


def draw_misfit(key, part):
    return ramped_field(key, 11)


def draw_multiplier(key, part):
    return ramped_field(key, 23)


def set_ends(values, rng, smallest, largest):
    dims = values.shape
    index_at = [jax.random.randint(jax.random.fold_in(rng, axis), (), 0, dims[axis]) for axis in range(len(dims))]
    values = values.at[tuple(index_at)].set(smallest)
    longest = dims.index(max(dims))
    index_at[longest] = (index_at[longest] + 1) % dims[longest]
    return values.at[tuple(index_at)].set(largest)


def block_levels(key, shape, pieces, low, top_value):
    level, own = 1.0, jax.random.fold_in(key, 6)
    for dim, shards_of in pieces:
        heights = jnp.exp(jax.random.uniform(jax.random.fold_in(own, dim), (shards_of,), jnp.float32, low / len(pieces), top_value / len(pieces)))
        level = level * jnp.repeat(heights, shape[dim] // shards_of).reshape([-1 if axis == dim else 1 for axis in range(len(shape))])
    return level


def normal_values(rng, shape, deviation, bound, shards=(), held_as=jnp.bfloat16):
    drawn = deviation * jax.random.normal(rng, shape, jnp.float32)
    if shards:
        drawn = drawn * block_levels(rng, shape, shards, -0.22, 0.18)
    return jnp.clip(drawn, -bound, bound).astype(held_as)


def setup_inputs(seed: int = 0) -> dict:
    key_list = jax.random.split(jax.random.key(seed), 11)
    increment = normal_values(key_list[0], (SUBWINDOWS, 5, LEV, NX, NY), 1.0, 6.0, ((0, 8), (3, 32)), jnp.float32)
    multiplier = draw_multiplier(jax.random.fold_in(key_list[10], 71), 0)
    sensor_multiplier = normal_values(key_list[2], (SUBWINDOWS, NOBS), 1.0, 6.0, ((0, 8),), jnp.float32)
    misfit = draw_misfit(jax.random.fold_in(key_list[10], 71), 0)
    innovation = normal_values(key_list[4], (SUBWINDOWS, NOBS), 1.0, 6.0, ((0, 8),), jnp.float32)
    model_error = jnp.clip(jnp.exp(jax.random.uniform(key_list[5], (5, LEV), jnp.float32, math.log(0.2), math.log(1.0))), 0.2, 1.0)
    sensor_error = jnp.clip(jnp.exp(math.log(1.5) - 1.60943787 * jax.random.uniform(key_list[6], (SUBWINDOWS, NOBS), jnp.float32) ** block_levels(key_list[6], (SUBWINDOWS, NOBS), ((0, 8),), -0.2, 0.2)), 0.3, 1.5)
    trajectory = jnp.clip(1.0 * jax.random.uniform(key_list[7], (SUBWINDOWS, STEPS, 2, LEV, NX, NY), jnp.float32) ** block_levels(key_list[7], (SUBWINDOWS, STEPS, 2, LEV, NX, NY), ((0, 8), (4, 32)), -0.2, 0.2), 0.0, 1.0).astype(jnp.bfloat16)
    land_sea = set_ends((jax.random.randint(key_list[8], (NX, NY), 0, 8) < 7).astype(jnp.int32), jax.random.fold_in(key_list[8], 1), 0, 1)
    sensor_cells = set_ends(jax.random.randint(key_list[9], (SUBWINDOWS, NOBS), 0, 2 * LEV * NX * NY), jax.random.fold_in(key_list[9], 1), 0, (2 * LEV * NX * NY) - 1).astype(jnp.int32)
    return {"increment": increment, "multiplier": multiplier, "sensor_multiplier": sensor_multiplier, "misfit": misfit, "innovation": innovation, "model_error": model_error, "sensor_error": sensor_error, "trajectory": trajectory, "land_sea": land_sea, "sensor_cells": sensor_cells}


thermal_lin = 0.2
thermal_quad = 0.02
haline_lin = 0.8
cabbeling = 0.01
gravity = 1.0
time_stride = 0.3
mixing = 0.15
coriolis = 0.5
relaxation = 0.5
epsilon = 1e-06

def column_pad(values):
    return jnp.pad(values, ((0, 0), (0, 0), (1, 1)))

def tendency(padded, history, landmask):
    temper = 30.0 * history[0] - 10.0
    saline = 8.0 * history[1] - 5.0
    dens_temper = -thermal_lin - thermal_quad * temper + cabbeling * saline
    dens_saline = haline_lin + cabbeling * temper
    density = dens_temper * padded[0] + dens_saline * padded[1]
    pressure = padded[4] + gravity * density
    latitude = padded.shape[3]
    rotation = coriolis * (jnp.arange(latitude, dtype=jnp.float32) - 0.5 * (latitude - 1)) / (0.5 * latitude)

    def middle(f):
        return f[:, 1:-1]

    def zonal_slope(f):
        return 0.5 * (f[:, 2:] - f[:, :-2])

    def meridional_slope(f):
        g = column_pad(middle(f))
        return 0.5 * (g[..., 2:] - g[..., :-2])

    def laplacian(f):
        g = column_pad(middle(f))
        return f[:, 2:] + f[:, :-2] + g[..., 2:] + g[..., :-2] - 4.0 * middle(f)
    heat_next = middle(padded[0]) + mixing * laplacian(padded[0])
    salt_next = middle(padded[1]) + mixing * laplacian(padded[1])
    east_next = middle(padded[2]) + time_stride * (rotation * middle(padded[3]) - zonal_slope(pressure))
    north_next = middle(padded[3]) + time_stride * (-rotation * middle(padded[2]) - meridional_slope(pressure))
    surface_next = middle(padded[4]) - time_stride * (zonal_slope(padded[2]) + meridional_slope(padded[3])) + mixing * laplacian(padded[4])
    return jnp.stack([heat_next, salt_next, east_next, north_next, surface_next]) * landmask

def wrap_columns(values):
    return jnp.concatenate([values[..., -1:, :], values, values[..., :1, :]], axis=-2)

def propagate(initial, history, landmask):
    fields = initial
    for j in range(STEPS):
        fields = tendency(wrap_columns(fields), wrap_columns(history[j]), landmask)
    return fields

def adjoint(cotangent, history, landmask):
    _, pull = jax.vjp(lambda v: propagate(v, history, landmask), jnp.zeros_like(cotangent))
    return pull(cotangent)[0]

def reference(increment, multiplier, sensor_multiplier, misfit, innovation, model_error, sensor_error, trajectory, land_sea, sensor_cells):
    landmask = land_sea.astype(jnp.float32)
    history = trajectory.astype(jnp.float32)
    forward = lax.map(lambda p: propagate(p[0], p[1], landmask), (increment, history))
    previous = jnp.concatenate([jnp.zeros_like(forward[:1]), forward[:-1]], axis=0)
    damping = model_error[None, :, :, None, None]
    model_residual = misfit - damping * multiplier - (increment - previous)
    multiplier_next = multiplier + relaxation * model_residual
    flattened = increment[:, :2].reshape(increment.shape[0], -1)
    observed = jnp.take_along_axis(flattened, sensor_cells, axis=1)
    sensor_residual = innovation - sensor_error * sensor_multiplier - observed
    sensor_next = sensor_multiplier + relaxation * sensor_residual
    following = jnp.concatenate([multiplier_next[1:], jnp.zeros_like(multiplier_next[:1])], axis=0)
    returned = lax.map(lambda p: adjoint(p[0], p[1], landmask), (following, history))
    subwindow_rows = jnp.arange(flattened.shape[0], dtype=jnp.int32)[:, None]
    spread = jnp.zeros_like(flattened).at[subwindow_rows, sensor_cells].add(sensor_next)
    spread = spread.reshape(increment[:, :2].shape)
    sensor_part = jnp.concatenate([spread, jnp.zeros_like(increment[:, 2:])], axis=1)
    gradient = multiplier_next - returned + sensor_part
    misfit_square = jnp.sum(model_residual * model_residual) + jnp.sum(sensor_residual * sensor_residual)
    gradient_square = jnp.sum(gradient * gradient)
    stride = misfit_square / (gradient_square + epsilon)
    return (increment - stride * gradient, multiplier_next, sensor_next)
```

```python
import functools

import jax
import jax.numpy as jnp
from jax import lax
from jax.experimental import pallas as pl
from jax.experimental.pallas import tpu as pltpu
from jax.sharding import PartitionSpec as P

MESH = pl.DeviceIdType.MESH
DIMS = (2, 4, 4, 4, 2)
CH = 16
F32 = jnp.float32
BF16 = jnp.bfloat16
NHALO = 13
LANES = 128


def sensor_kernel(
    inc_ref, cell_ref, inno_ref, serr_ref, smul_ref, spread_ref, obs_ref, ssum_ref, ft, acc
):
    subcount, nobs = cell_ref.shape
    rows = ft.shape[1]
    width = 8
    block = 256
    columns = width * lax.axis_size("space")
    offset = lax.axis_index("space") * width
    row_id = lax.broadcasted_iota(jnp.int32, (rows, block), 0)
    lane_id = lax.broadcasted_iota(jnp.int32, (LANES, block), 0)
    total = jnp.zeros((1, block), F32)
    for k in range(subcount):
        flat = inc_ref[k].reshape(rows, LANES)
        turned = flat.T
        high = turned.astype(BF16)
        ft[0:LANES, :] = high
        ft[LANES:, :] = (turned - high.astype(F32)).astype(BF16)
        acc[...] = jnp.zeros_like(acc)

        def chunk(n, total):
            at = pl.ds(pl.multiple_of(n * block, block), block)
            cell = cell_ref[k : k + 1, at]
            row = cell & (LANES - 1)
            rest = cell >> 7
            col = rest & (columns - 1)
            level = rest >> (columns.bit_length() - 1)
            own = (col >= offset) & (col < offset + width)
            local = jnp.where(own, level * width + col - offset, -1)
            hot = jnp.where(row_id == local, 1.0, 0.0).astype(BF16)
            lane = lane_id == row
            picked = jnp.dot(ft[...], hot, preferred_element_type=F32)
            both = picked[:LANES] + picked[LANES:]
            obs = jnp.sum(jnp.where(lane, both, 0.0), axis=0, keepdims=True)
            smul = smul_ref[k : k + 1, at]
            res = inno_ref[k : k + 1, at] - serr_ref[k : k + 1, at] * smul - obs
            nxt = smul + 0.5 * res
            put = jnp.where(lane, nxt, 0.0)
            put_high = put.astype(BF16)
            put_low = (put - put_high.astype(F32)).astype(BF16)
            put2 = jnp.concatenate([put_high, put_low], axis=0)
            acc[...] += lax.dot_general(
                hot, put2, (((1,), (1,)), ((), ())), preferred_element_type=F32
            )
            obs_ref[k : k + 1, at] = obs
            return total + jnp.where(own, res * res, 0.0)

        total = lax.fori_loop(0, nobs // block, chunk, total)
        both = acc[:, :LANES] + acc[:, LANES:]
        spread_ref[k] = both.reshape(spread_ref.shape[1:])
    ssum_ref[...] = total[:, :LANES] + total[:, LANES:]


def main_kernel(
    dims,
    inc_h, mul_h, mis_h, traj_h, land, damp, spread, obs_in, ssum,
    g_h, mn_h, obs_out, sum_out,
    inc_n, mul_n, mis_n, traj_n, g_n, mn_n,
    x, kt, ks, q0, y, q1, fw, r0, wa, wb, rt, mm, kn,
    hs, hr, f_send, f_recv, b_send, b_recv, macc, gacc,
    so, so_recv, ar, ar_recv,
    in_sem, out_sem, send_sem, recv_sem,
):
    zh_n, x_n, y_n, zl_n, c_n = dims
    tm = lax.axis_index("tm")
    sp = lax.axis_index("space")
    tm_n = zh_n * x_n
    sp_n = y_n * zl_n * c_n
    zh, xx = tm // x_n, tm % x_n
    yy, zl, cc = sp // (zl_n * c_n), (sp // c_n) % zl_n, sp % c_n
    levels = x.shape[3]
    chunks = levels // CH
    left = (tm, (sp + sp_n - 1) % sp_n)
    right = (tm, (sp + 1) % sp_n)
    first, last = tm == 0, tm == tm_n - 1

    def at_space(dy, dz, dc):
        return (
            ((yy + dy) % y_n) * (zl_n * c_n) + ((zl + dz) % zl_n) * c_n + (cc + dc) % c_n
        )

    group_a = [(tm, at_space(dy, 0, dc)) for dy in range(y_n) for dc in range(c_n) if dy or dc]
    group_b = [(zh * x_n + (xx + dx) % x_n, sp) for dx in range(1, x_n)]
    z_n = zh_n * zl_n
    group_c = []
    for dz in range(1, z_n):
        z = (zh * zl_n + zl + dz) % z_n
        group_c.append(
            ((z // zl_n) * x_n + xx, yy * (zl_n * c_n) + (z % zl_n) * c_n + cc)
        )
    obs_y = [(tm, at_space(dy, 0, 0)) for dy in range(1, y_n)]
    obs_z = [(tm, at_space(0, dz, 0)) for dz in range(1, zl_n)]
    obs_c = [(tm, at_space(0, 0, dc)) for dc in range(1, c_n)]

    loads = {}

    def load(name, src, dst, n):
        copy = pltpu.make_async_copy(src, dst, in_sem.at[n])
        copy.start()
        loads[name] = copy

    load("inc0", inc_h.at[0], inc_n.at[0], 0)
    load("mul0", mul_h.at[0], mul_n.at[0], 1)
    load("mis0", mis_h.at[0], mis_n.at[0], 2)
    load("inc1", inc_h.at[1], inc_n.at[1], 3)
    load("traj", traj_h, traj_n, 4)
    load("mul1", mul_h.at[1], mul_n.at[1], 5)
    load("mis1", mis_h.at[1], mis_n.at[1], 6)

    barrier = pltpu.get_barrier_semaphore()
    everyone = [left, right] + group_a + group_b + group_c + obs_y + obs_z + obs_c
    for peer in everyone:
        pl.semaphore_signal(barrier, inc=1, device_id=peer, device_id_type=MESH)

    @pl.when(tm > 0)
    def _():
        pl.semaphore_signal(barrier, inc=1, device_id=(tm - 1, sp), device_id_type=MESH)

    @pl.when(tm < tm_n - 1)
    def _():
        pl.semaphore_signal(barrier, inc=1, device_id=(tm + 1, sp), device_id_type=MESH)

    sem_n = [0]

    def remote(src, dst, peer):
        n = sem_n[0]
        sem_n[0] += 1
        return pltpu.make_async_remote_copy(
            src_ref=src, dst_ref=dst, send_sem=send_sem.at[n], recv_sem=recv_sem.at[n],
            device_id=peer, device_id_type=MESH,
        )

    lane = lax.broadcasted_iota(jnp.int32, (CH, LANES), 1)
    c_dn = jnp.where(lane > 0, 0.15, 0.0)
    c_up = jnp.where(lane < LANES - 1, 0.15, 0.0)
    r3 = (0.3 * 0.5 / (0.5 * LANES)) * (lane.astype(F32) - 0.5 * (LANES - 1))

    def dn(v):
        return c_dn * pltpu.roll(v, 1, 1)

    def up(v):
        return c_up * pltpu.roll(v, LANES - 1, 1)

    def over_chunks(body, init=None):
        def step(n, carry):
            return body(pl.multiple_of(n * CH, CH), carry)

        return lax.fori_loop(0, chunks, step, init)

    def nat(l0, c):
        return pl.ds(l0 * 8 + c, CH, stride=8)

    def lv(l0):
        return pl.ds(l0, CH)

    for c in range(8):
        mm[c + 2] = jnp.broadcast_to(land[c : c + 1, :].astype(F32), (CH, LANES))
    zero = jnp.zeros((CH, LANES), F32)
    macc[...] = zero
    gacc[...] = zero

    def residual(k, with_send):
        def body(l0, _):
            for f in range(5):
                d = damp[f, lv(l0), :]
                for c in range(8):
                    mu = mul_n[k, f, nat(l0, c), :]
                    v = inc_n[k, f, nat(l0, c), :]
                    r = mis_n[k, f, nat(l0, c), :] - d * mu - v
                    r0[k, f, c, lv(l0), :] = r
                    if with_send:
                        b_send[f, c, lv(l0), :] = (mu + 0.5 * r).astype(BF16)
            return _

        over_chunks(body, 0)

    loads["inc0"].wait()
    loads["mul0"].wait()
    loads["mis0"].wait()
    residual(0, True)

    n_edge = jnp.where(first, 0, 1) + jnp.where(last, 0, 1)
    pl.semaphore_wait(barrier, len(everyone) + n_edge)

    b_copy = remote(b_send, b_recv, (lax.rem(tm + tm_n - 1, tm_n), sp))

    @pl.when(tm > 0)
    def _():
        b_copy.start()

    @pl.when(last)
    def _():
        b_recv[...] = jnp.zeros_like(b_recv)

    @pl.when(first)
    def _():
        f_recv[...] = jnp.zeros_like(f_recv)

    def prepare(k):
        def body(l0, _):
            for j in range(2):
                h0 = traj_n[k, j, 0, pl.ds(l0 * 8, 8 * CH), :].astype(F32)
                h1 = traj_n[k, j, 1, pl.ds(l0 * 8, 8 * CH), :].astype(F32)
                kn[0] = -0.6 * h0 + 0.08 * h1 - 0.05
                kn[1] = 0.7 + 0.3 * h0
                for c in range(8):
                    kt[k, j, c + 2, lv(l0), :] = kn[0, pl.ds(c, CH, stride=8), :]
                    ks[k, j, c + 2, lv(l0), :] = kn[1, pl.ds(c, CH, stride=8), :]
            for c in range(8):
                v = [inc_n[k, f, nat(l0, c), :] for f in range(5)]
                for f in range(5):
                    x[k, f, c + 2, lv(l0), :] = v[f]
                q = (
                    v[4]
                    + kt[k, 0, c + 2, lv(l0), :] * v[0]
                    + ks[k, 0, c + 2, lv(l0), :] * v[1]
                )
                q0[k, c + 2, lv(l0), :] = q
                for side, near, far in ((0, 0, 1), (1, 7, 6)):
                    out = []
                    if c == near:
                        out = list(enumerate(v + [q])) + [
                            (6, kt[k, 1, c + 2, lv(l0), :]),
                            (7, ks[k, 1, c + 2, lv(l0), :]),
                            (8, mm[c + 2]),
                        ]
                    if c == far:
                        pu = v[4] - v[2] if side == 0 else v[4] + v[2]
                        out = [(9, v[0]), (10, v[1]), (11, pu), (12, q)]
                    for n, value in out:
                        hs[k, side, n, lv(l0), :] = value.astype(BF16)
            return _

        over_chunks(body, 0)

    def send_halo(k):
        copies = [
            remote(hs.at[k, 0], hr.at[k, 1], left),
            remote(hs.at[k, 1], hr.at[k, 0], right),
        ]
        for copy in copies:
            copy.start()
        return copies

    loads["inc1"].wait()
    loads["traj"].wait()
    prepare(1)
    halo1 = send_halo(1)
    prepare(0)
    halo0 = send_halo(0)

    so[0] = obs_in[...]
    slot = [0]

    def obs_stage(stage, peers):
        copies = []
        for peer in peers:
            copies.append((remote(so.at[stage], so_recv.at[slot[0]], peer), slot[0]))
            copies[-1][0].start()
            slot[0] += 1
        return copies

    def obs_sum(stage, copies):
        value = so[stage]
        for copy, n in copies:
            copy.wait()
            value = value + so_recv[n]
        return value

    obs1 = obs_stage(0, obs_y)

    loads["mul1"].wait()
    loads["mis1"].wait()
    residual(1, False)

    def unpack(k, copies):
        for copy in copies:
            copy.wait()

        def body(l0, _):
            for side, near, far in ((0, 1, 0), (1, 10, 11)):

                def got(n):
                    return hr[k, side, n, lv(l0), :].astype(F32)

                for f in range(5):
                    x[k, f, near, lv(l0), :] = got(f)
                q0[k, near, lv(l0), :] = got(5)
                kt[k, 1, near, lv(l0), :] = got(6)
                ks[k, 1, near, lv(l0), :] = got(7)
                mm[near] = got(8)
                x[k, 0, far, lv(l0), :] = got(9)
                x[k, 1, far, lv(l0), :] = got(10)
                x[k, 2, far, lv(l0), :] = zero
                x[k, 4, far, lv(l0), :] = got(11)
                q0[k, far, lv(l0), :] = got(12)
            return _

        over_chunks(body, 0)

    def tangent(s, q, k, i, l0, m):
        def at(f, n):
            return s[k, f, n, lv(l0), :]

        t, sa, u, v, p = [at(f, i) for f in range(5)]
        qc = q[k, i, lv(l0), :]
        t2 = 0.4 * t + 0.15 * (at(0, i - 1) + at(0, i + 1)) + dn(t) + up(t)
        s2 = 0.4 * sa + 0.15 * (at(1, i - 1) + at(1, i + 1)) + dn(sa) + up(sa)
        u2 = u + r3 * v - 0.15 * (q[k, i + 1, lv(l0), :] - q[k, i - 1, lv(l0), :])
        v2 = v - r3 * u + dn(qc) - up(qc)
        east = at(4, i + 1) - at(2, i + 1)
        west = at(4, i - 1) + at(2, i - 1)
        p2 = 0.4 * p + 0.15 * (east + west) + up(p - v) + dn(p + v)
        return [m * w for w in (t2, s2, u2, v2, p2)]

    def first_substep(k):
        def body(l0, _):
            for i in range(1, 11):
                new = tangent(x, q0, k, i, l0, mm[i])
                for f in range(5):
                    y[k, f, i - 1, lv(l0), :] = new[f]
                q1[k, i - 1, lv(l0), :] = (
                    new[4] + kt[k, 1, i, lv(l0), :] * new[0] + ks[k, 1, i, lv(l0), :] * new[1]
                )
            return _

        over_chunks(body, 0)

    def second_substep(k):
        def body(l0, acc):
            for i in range(1, 9):
                c = i - 1
                m = mm[c + 2]
                new = tangent(y, q1, k, i, l0, m)
                for f in range(5):
                    if k == 1:
                        fw[f, c, lv(l0), :] = new[f]
                        f_send[f, c, lv(l0), :] = new[f].astype(BF16)
                    else:
                        r = r0[1, f, c, lv(l0), :] + new[f]
                        acc = acc + r * r
                        mn = mul_n[1, f, nat(l0, c), :] + 0.5 * r
                        mn_n[1, f, nat(l0, c), :] = mn
                        wa[0, f, c + 2, lv(l0), :] = m * mn
            return acc

        macc[...] = over_chunks(body, macc[...])

    unpack(1, halo1)
    first_substep(1)
    second_substep(1)
    f_copy = remote(f_send, f_recv, (lax.rem(tm + 1, tm_n), sp))

    @pl.when(tm < tm_n - 1)
    def _():
        f_copy.start()

    unpack(0, halo0)
    first_substep(0)
    second_substep(0)

    def send_edges(k):
        copies = [
            remote(wa.at[k, :, 2:4], wa.at[k, :, 10:12], left),
            remote(wa.at[k, :, 8:10], wa.at[k, :, 0:2], right),
        ]
        for copy in copies:
            copy.start()
        return copies

    edges0 = send_edges(0)
    outs = []

    def store(src, dst, n):
        copy = pltpu.make_async_copy(src, dst, out_sem.at[n])
        copy.start()
        outs.append(copy)

    store(mn_n.at[1], mn_h.at[1], 0)

    so[1] = obs_sum(0, obs1)
    obs2 = obs_stage(1, obs_z)

    @pl.when(tm < tm_n - 1)
    def _():
        b_copy.wait_recv()

    keep = jnp.where(last, 0.0, 1.0)

    def following(l0, _):
        for c in range(8):
            m = keep * mm[c + 2]
            for f in range(5):
                u = b_recv[f, c, lv(l0), :].astype(F32) + 0.5 * fw[f, c, lv(l0), :]
                wa[1, f, c + 2, lv(l0), :] = m * u
        return _

    over_chunks(following, 0)
    edges1 = send_edges(1)

    def transposed(s, k, j, i, col, l0):
        def at(f, n):
            return s[k, f, n, lv(l0), :]

        t, sa, u, v, p = [at(f, i) for f in range(5)]
        pw, pe = at(4, i - 1), at(4, i + 1)
        q = 0.15 * (at(2, i + 1) - at(2, i - 1)) + up(v) - dn(v)
        t2 = 0.4 * t + 0.15 * (at(0, i - 1) + at(0, i + 1)) + dn(t) + up(t)
        t2 = t2 + kt[k, j, col, lv(l0), :] * q
        s2 = 0.4 * sa + 0.15 * (at(1, i - 1) + at(1, i + 1)) + dn(sa) + up(sa)
        s2 = s2 + ks[k, j, col, lv(l0), :] * q
        south, north = dn(p), up(p)
        u2 = u - r3 * v + 0.15 * (pe - pw)
        v2 = v + r3 * u + north - south
        p2 = 0.4 * p + 0.15 * (pe + pw) + south + north + q
        return [t2, s2, u2, v2, p2]

    def first_transposed(k):
        def body(l0, _):
            for i in range(1, 11):
                new = transposed(wa, k, 1, i, i, l0)
                m = mm[i]
                for f in range(5):
                    wb[k, f, i - 1, lv(l0), :] = m * new[f]
            return _

        over_chunks(body, 0)

    def second_transposed(k):
        def body(l0, acc):
            for i in range(1, 9):
                c = i - 1
                new = transposed(wb, k, 0, i, c + 2, l0)
                for f in range(5):
                    if k == 0:
                        rt[f, c, lv(l0), :] = new[f]
                    else:
                        g = mn_n[1, f, nat(l0, c), :] - new[f]
                        if f < 2:
                            g = g + spread[1, f, nat(l0, c), :]
                        g_n[1, f, nat(l0, c), :] = g
                        acc = acc + g * g
            return acc

        gacc[...] = over_chunks(body, gacc[...])

    for copy in edges0:
        copy.wait()
    first_transposed(0)
    second_transposed(0)

    so[2] = obs_sum(1, obs2)
    obs3 = obs_stage(2, obs_c)

    for copy in edges1:
        copy.wait()
    first_transposed(1)
    second_transposed(1)
    store(g_n.at[1], g_h.at[1], 1)

    @pl.when(tm > 0)
    def _():
        f_copy.wait_recv()

    def finish(l0, carry):
        ma, ga = carry
        for f in range(5):
            for c in range(8):
                r = r0[0, f, c, lv(l0), :] + f_recv[f, c, lv(l0), :].astype(F32)
                ma = ma + r * r
                mn = mul_n[0, f, nat(l0, c), :] + 0.5 * r
                mn_n[0, f, nat(l0, c), :] = mn
                g = mn - rt[f, c, lv(l0), :]
                if f < 2:
                    g = g + spread[0, f, nat(l0, c), :]
                g_n[0, f, nat(l0, c), :] = g
                ga = ga + g * g
        return ma, ga

    ma, ga = over_chunks(finish, (macc[...], gacc[...]))
    ma = jnp.sum(ma, axis=0, keepdims=True) + ssum[...]
    ga = jnp.sum(ga, axis=0, keepdims=True)
    sub = lax.broadcasted_iota(jnp.int32, (8, LANES), 0)
    value = jnp.where(sub == 0, ma, jnp.where(sub == 1, ga, 0.0))

    pending = []
    n = 0
    for stage, peers in enumerate((group_a, group_b, group_c)):
        ar[stage] = value
        copies = []
        for peer in peers:
            copies.append((remote(ar.at[stage], ar_recv.at[n], peer), n))
            copies[-1][0].start()
            n += 1
        if stage == 0:
            store(g_n.at[0], g_h.at[0], 2)
            store(mn_n.at[0], mn_h.at[0], 3)
            obs_out[...] = obs_sum(2, obs3)
        for copy, m in copies:
            copy.wait_recv()
            value = value + ar_recv[m]
        pending += [copy for copy, _ in copies]
    sum_out[...] = value

    for copy in pending:
        copy.wait_send()

    @pl.when(tm > 0)
    def _():
        b_copy.wait_send()

    @pl.when(tm < tm_n - 1)
    def _():
        f_copy.wait_send()

    for copy in outs:
        copy.wait()


def on_device(
    dims,
    increment,
    multiplier,
    sensor_multiplier,
    misfit,
    innovation,
    model_error,
    sensor_error,
    trajectory,
    land_sea,
    sensor_cells,
):
    subcount, fields, levels, width, latitude = increment.shape
    rows = levels * width
    nobs = sensor_cells.shape[1]
    zh_n, x_n, y_n, zl_n, c_n = dims
    flat = (subcount, fields, rows, latitude)
    vmem = pl.BlockSpec(memory_space=pltpu.VMEM)
    hbm = pl.BlockSpec(memory_space=pltpu.HBM)

    inc = increment.reshape(flat)
    spread, obs, ssum = pl.pallas_call(
        sensor_kernel,
        grid=(1,),
        out_shape=(
            jax.ShapeDtypeStruct((subcount, 2, rows, latitude), F32),
            jax.ShapeDtypeStruct((subcount, nobs), F32),
            jax.ShapeDtypeStruct((1, latitude), F32),
        ),
        in_specs=[pl.BlockSpec((subcount, 2, rows, latitude), lambda i: (0, 0, 0, 0))]
        + [pl.BlockSpec((subcount, nobs), lambda i: (0, 0))] * 4,
        out_specs=(
            pl.BlockSpec((subcount, 2, rows, latitude), lambda i: (0, 0, 0, 0)),
            pl.BlockSpec((subcount, nobs), lambda i: (0, 0)),
            pl.BlockSpec((1, latitude), lambda i: (0, 0)),
        ),
        scratch_shapes=[
            pltpu.VMEM((2 * LANES, 2 * rows), BF16),
            pltpu.VMEM((2 * rows, 2 * LANES), F32),
        ],
        compiler_params=pltpu.CompilerParams(vmem_limit_bytes=40 << 20),
        name="sensors",
    )(inc, sensor_cells, innovation, sensor_error, sensor_multiplier)

    damp = jnp.broadcast_to(model_error[:, :, None], (fields, levels, latitude))
    n_obs = (y_n - 1) + (zl_n - 1) + (c_n - 1)
    n_ar = (y_n * c_n - 1) + (x_n - 1) + (zh_n * zl_n - 1)
    n_sem = 10 + n_obs + n_ar

    def v(*shape, dtype=F32):
        return pltpu.VMEM(shape, dtype)

    lr = (levels, latitude)
    grad, mult_next, observed, sums = pl.pallas_call(
        functools.partial(main_kernel, dims),
        out_shape=(
            jax.ShapeDtypeStruct(flat, F32),
            jax.ShapeDtypeStruct(flat, F32),
            jax.ShapeDtypeStruct((subcount, nobs), F32),
            jax.ShapeDtypeStruct((8, latitude), F32),
        ),
        in_specs=[hbm] * 4 + [vmem] * 5,
        out_specs=(hbm, hbm, vmem, vmem),
        scratch_shapes=[
            v(*flat), v(*flat), v(*flat),
            v(subcount, 2, 2, rows, latitude, dtype=BF16),
            v(*flat), v(*flat),
            v(subcount, fields, 12, *lr),
            v(subcount, 2, 12, *lr), v(subcount, 2, 12, *lr),
            v(subcount, 12, *lr),
            v(subcount, fields, 10, *lr),
            v(subcount, 10, *lr),
            v(fields, 8, *lr),
            v(subcount, fields, 8, *lr),
            v(subcount, fields, 12, *lr),
            v(subcount, fields, 10, *lr),
            v(fields, 8, *lr),
            v(12, CH, latitude),
            v(2, 8 * CH, latitude),
            v(subcount, 2, NHALO, *lr, dtype=BF16),
            v(subcount, 2, NHALO, *lr, dtype=BF16),
            v(fields, 8, *lr, dtype=BF16), v(fields, 8, *lr, dtype=BF16),
            v(fields, 8, *lr, dtype=BF16), v(fields, 8, *lr, dtype=BF16),
            v(CH, latitude), v(CH, latitude),
            v(3, subcount, nobs), v(n_obs, subcount, nobs),
            v(3, 8, latitude), v(n_ar, 8, latitude),
            pltpu.SemaphoreType.DMA((7,)),
            pltpu.SemaphoreType.DMA((4,)),
            pltpu.SemaphoreType.DMA((n_sem,)),
            pltpu.SemaphoreType.DMA((n_sem,)),
        ],
        compiler_params=pltpu.CompilerParams(
            vmem_limit_bytes=52 << 20, collective_id=0, has_side_effects=True
        ),
        name="uzawa",
    )(
        inc,
        multiplier.reshape(flat),
        misfit.reshape(flat),
        trajectory.reshape(subcount, 2, 2, rows, latitude),
        land_sea,
        damp,
        spread,
        obs,
        ssum,
    )
    stride = jnp.sum(sums[0]) / (jnp.sum(sums[1]) + 1e-6)
    sensor_residual = innovation - sensor_error * sensor_multiplier - observed
    return (
        increment - stride * grad.reshape(increment.shape),
        mult_next.reshape(increment.shape),
        sensor_multiplier + 0.5 * sensor_residual,
    )


def solution(mesh, dims=DIMS):
    return jax.shard_map(
        functools.partial(on_device, dims),
        mesh=mesh,
        in_specs=(
            P("tm", None, None, "space", None),
            P("tm", None, None, "space", None),
            P("tm", None),
            P("tm", None, None, "space", None),
            P("tm", None),
            P(),
            P("tm", None),
            P("tm", None, None, None, "space", None),
            P("space", None),
            P("tm", None),
        ),
        out_specs=(
            P("tm", None, None, "space", None),
            P("tm", None, None, "space", None),
            P("tm", None),
        ),
        check_vma=False,
    )
```

```python
import functools

import jax
import jax.numpy as jnp
from jax import lax
from jax.experimental import pallas as pl
from jax.experimental.pallas import tpu as pltpu
from jax.sharding import PartitionSpec as P

MESH = pl.DeviceIdType.MESH
DIMS = (2, 4, 4, 4, 2)
CH = 16
F32 = jnp.float32
BF16 = jnp.bfloat16
NHALO = 13
NEDGE = 9
LANES = 128


def main_kernel(
    dims,
    inc_h, mul_h, mis_h, traj_h, land_h, damp_h, cell_h, inno_h, serr_h, smul_h,
    inc_out, mn_out, sens_out,
    inc_n, mul_n, mis_n, traj_n, g_n, mn_n, sens_n,
    land, damp5, cell_v, inno_v, serr_v, smul_v, damp, spread, ft, acc2,
    x, kt, ks, q0, y, q1, fw, r0, wa, wb, rt, mm, kn,
    hs, hr, es, er, f_send, f_recv, b_send, b_recv, macc, gacc,
    so, so_recv, ar, ar_recv,
    in_sem, out_sem, send_sem, recv_sem,
):
    zh_n, x_n, y_n, zl_n, c_n = dims
    tm = lax.axis_index("tm")
    sp = lax.axis_index("space")
    tm_n = zh_n * x_n
    sp_n = y_n * zl_n * c_n
    zh, xx = tm // x_n, tm % x_n
    yy, zl, cc = sp // (zl_n * c_n), (sp // c_n) % zl_n, sp % c_n
    levels = x.shape[3]
    chunks = levels // CH
    left = (tm, (sp + sp_n - 1) % sp_n)
    right = (tm, (sp + 1) % sp_n)
    first, last = tm == 0, tm == tm_n - 1

    def at_space(dy, dz, dc):
        return (
            ((yy + dy) % y_n) * (zl_n * c_n) + ((zl + dz) % zl_n) * c_n + (cc + dc) % c_n
        )

    group_a = [(tm, at_space(dy, 0, dc)) for dy in range(y_n) for dc in range(c_n) if dy or dc]
    group_b = [(zh * x_n + (xx + dx) % x_n, sp) for dx in range(1, x_n)]
    z_n = zh_n * zl_n
    group_c = []
    for dz in range(1, z_n):
        z = (zh * zl_n + zl + dz) % z_n
        group_c.append(
            ((z // zl_n) * x_n + xx, yy * (zl_n * c_n) + (z % zl_n) * c_n + cc)
        )
    obs_y = [(tm, at_space(dy, 0, 0)) for dy in range(1, y_n)]
    obs_z = [(tm, at_space(0, dz, 0)) for dz in range(1, zl_n)]
    obs_c = [(tm, at_space(0, 0, dc)) for dc in range(1, c_n)]

    loads = {}

    def load(name, src, dst, n):
        copy = pltpu.make_async_copy(src, dst, in_sem.at[n])
        copy.start()
        loads[name] = copy

    n_in = inc_n.shape[0] // 2

    def part(k):
        return pl.ds(k * n_in, n_in)

    load("inc1", inc_h.at[part(1)], inc_n.at[part(1)], 0)
    load("traj", traj_h, traj_n, 1)
    load("land", land_h, land, 2)
    load("damp", damp_h, damp5, 3)
    load("inc0", inc_h.at[part(0)], inc_n.at[part(0)], 4)
    load("mul0", mul_h.at[part(0)], mul_n.at[part(0)], 5)
    load("mis0", mis_h.at[part(0)], mis_n.at[part(0)], 6)
    load("cell", cell_h, cell_v, 7)
    load("inno", inno_h, inno_v, 8)
    load("serr", serr_h, serr_v, 9)
    load("smul", smul_h, smul_v, 10)
    load("mul1", mul_h.at[part(1)], mul_n.at[part(1)], 11)
    load("mis1", mis_h.at[part(1)], mis_n.at[part(1)], 12)

    barrier = pltpu.get_barrier_semaphore()
    everyone = [left, right] + group_a + group_b + group_c + obs_y + obs_z + obs_c
    for peer in everyone:
        pl.semaphore_signal(barrier, inc=1, device_id=peer, device_id_type=MESH)

    @pl.when(tm > 0)
    def _():
        pl.semaphore_signal(barrier, inc=1, device_id=(tm - 1, sp), device_id_type=MESH)

    @pl.when(tm < tm_n - 1)
    def _():
        pl.semaphore_signal(barrier, inc=1, device_id=(tm + 1, sp), device_id_type=MESH)

    sem_n = [0]

    def remote(src, dst, peer):
        n = sem_n[0]
        sem_n[0] += 1
        return pltpu.make_async_remote_copy(
            src_ref=src, dst_ref=dst, send_sem=send_sem.at[n], recv_sem=recv_sem.at[n],
            device_id=peer, device_id_type=MESH,
        )

    lane = lax.broadcasted_iota(jnp.int32, (CH, LANES), 1)
    c_dn = jnp.where(lane > 0, 0.15, 0.0)
    c_up = jnp.where(lane < LANES - 1, 0.15, 0.0)
    r3 = (0.3 * 0.5 / (0.5 * LANES)) * (lane.astype(F32) - 0.5 * (LANES - 1))

    def dn(v):
        return c_dn * pltpu.roll(v, 1, 1)

    def up(v):
        return c_up * pltpu.roll(v, LANES - 1, 1)

    def over_chunks(body, init=None):
        def step(n, carry):
            return body(pl.multiple_of(n * CH, CH), carry)

        return lax.fori_loop(0, chunks, step, init)

    def nat(l0, c):
        return pl.ds(l0 * 8 + c, CH, stride=8)

    def lv(l0):
        return pl.ds(l0, CH)

    zero = jnp.zeros((CH, LANES), F32)
    macc[...] = zero
    gacc[...] = zero

    def constants():
        for c in range(8):
            mm[c + 2] = jnp.broadcast_to(land[c : c + 1, :].astype(F32), (CH, LANES))
        same = lax.broadcasted_iota(jnp.int32, (levels, levels), 0) == (
            lax.broadcasted_iota(jnp.int32, (levels, levels), 1)
        )
        for f in range(5):
            spot = jnp.where(same, damp5[f : f + 1, :], 0.0)
            damp[f] = jnp.broadcast_to(jnp.sum(spot, axis=1, keepdims=True), (levels, LANES))

    def residual(k, with_send):
        def body(l0, _):
            for f in range(5):
                d = damp[f, lv(l0), :]
                for c in range(8):
                    mu = mul_n[k * 5 + f, nat(l0, c), :]
                    v = inc_n[k * 5 + f, nat(l0, c), :]
                    r = mis_n[k * 5 + f, nat(l0, c), :] - d * mu - v
                    r0[k, f, c, lv(l0), :] = r
                    if with_send:
                        b_send[f, c, lv(l0), :] = (mu + 0.5 * r).astype(BF16)
            return _

        over_chunks(body, 0)

    def prepare(k):
        def body(l0, _):
            for j in range(2):
                h0 = traj_n[k, j, 0, pl.ds(l0 * 8, 8 * CH), :].astype(F32)
                h1 = traj_n[k, j, 1, pl.ds(l0 * 8, 8 * CH), :].astype(F32)
                kn[0] = -0.6 * h0 + 0.08 * h1 - 0.05
                kn[1] = 0.7 + 0.3 * h0
                for c in range(8):
                    kt[k, j, c + 2, lv(l0), :] = kn[0, pl.ds(c, CH, stride=8), :]
                    ks[k, j, c + 2, lv(l0), :] = kn[1, pl.ds(c, CH, stride=8), :]
            for c in range(8):
                v = [inc_n[k * 5 + f, nat(l0, c), :] for f in range(5)]
                for f in range(5):
                    x[k, f, c + 2, lv(l0), :] = v[f]
                q = (
                    v[4]
                    + kt[k, 0, c + 2, lv(l0), :] * v[0]
                    + ks[k, 0, c + 2, lv(l0), :] * v[1]
                )
                q0[k, c + 2, lv(l0), :] = q
                for side, near, far in ((0, 0, 1), (1, 7, 6)):
                    out = []
                    if c == near:
                        out = list(enumerate(v + [q])) + [
                            (6, kt[k, 1, c + 2, lv(l0), :]),
                            (7, ks[k, 1, c + 2, lv(l0), :]),
                            (8, mm[c + 2]),
                        ]
                    if c == far:
                        pu = v[4] - v[2] if side == 0 else v[4] + v[2]
                        out = [(9, v[0]), (10, v[1]), (11, pu), (12, q)]
                    for n, value in out:
                        hs[k, side, n, lv(l0), :] = value.astype(BF16)
            return _

        over_chunks(body, 0)

    def send_halo(k):
        copies = [
            remote(hs.at[k, 0], hr.at[k, 1], left),
            remote(hs.at[k, 1], hr.at[k, 0], right),
        ]
        for copy in copies:
            copy.start()
        return copies

    for name in ("inc1", "traj", "land", "damp"):
        loads[name].wait()
    constants()
    prepare(1)
    for name in ("inc0", "mul0", "mis0"):
        loads[name].wait()
    residual(0, True)

    n_edge = jnp.where(first, 0, 1) + jnp.where(last, 0, 1)
    pl.semaphore_wait(barrier, len(everyone) + n_edge)
    halo1 = send_halo(1)

    b_copy = remote(b_send, b_recv, (lax.rem(tm + tm_n - 1, tm_n), sp))

    @pl.when(tm > 0)
    def _():
        b_copy.start()

    @pl.when(last)
    def _():
        b_recv[...] = jnp.zeros_like(b_recv)

    @pl.when(first)
    def _():
        f_recv[...] = jnp.zeros_like(f_recv)

    prepare(0)
    halo0 = send_halo(0)

    subcount, nobs = cell_v.shape
    rows = ft.shape[1]
    block = 256
    columns = 8 * sp_n
    offset = sp * 8
    row_id = lax.broadcasted_iota(jnp.int32, (rows, block), 0)
    lane_id = lax.broadcasted_iota(jnp.int32, (LANES, block), 0)

    def sensors(k, total):
        turned = inc_n[k * 5 : k * 5 + 2].reshape(rows, LANES).T
        high = turned.astype(BF16)
        ft[0:LANES, :] = high
        ft[LANES:, :] = (turned - high.astype(F32)).astype(BF16)
        acc2[...] = jnp.zeros_like(acc2)

        def chunk(n, total):
            at = pl.ds(pl.multiple_of(n * block, block), block)
            cell = cell_v[k : k + 1, at]
            row = cell & (LANES - 1)
            rest = cell >> 7
            col = rest & (columns - 1)
            level = rest >> (columns.bit_length() - 1)
            own = (col >= offset) & (col < offset + 8)
            local = jnp.where(own, level * 8 + col - offset, -1)
            hot = jnp.where(row_id == local, 1.0, 0.0).astype(BF16)
            on_lane = lane_id == row
            picked = jnp.dot(ft[...], hot, preferred_element_type=F32)
            both = picked[:LANES] + picked[LANES:]
            obs = jnp.sum(jnp.where(on_lane, both, 0.0), axis=0, keepdims=True)
            smul = smul_v[k : k + 1, at]
            res = inno_v[k : k + 1, at] - serr_v[k : k + 1, at] * smul - obs
            put = jnp.where(on_lane, smul + 0.5 * res, 0.0)
            put_high = put.astype(BF16)
            put_low = (put - put_high.astype(F32)).astype(BF16)
            put2 = jnp.concatenate([put_high, put_low], axis=0)
            acc2[...] += lax.dot_general(
                hot, put2, (((1,), (1,)), ((), ())), preferred_element_type=F32
            )
            so[0, k : k + 1, at] = obs
            return total + jnp.where(own, res * res, 0.0)

        total = lax.fori_loop(0, nobs // block, chunk, total)
        both = acc2[:, :LANES] + acc2[:, LANES:]
        spread[k] = both.reshape(spread.shape[1:])
        return total

    for name in ("cell", "inno", "serr", "smul", "mul1", "mis1"):
        loads[name].wait()
    residual(1, False)
    total = sensors(1, jnp.zeros((1, block), F32))

    slot = [0]

    def obs_stage(stage, peers):
        copies = []
        for peer in peers:
            copies.append((remote(so.at[stage], so_recv.at[slot[0]], peer), slot[0]))
            copies[-1][0].start()
            slot[0] += 1
        return copies

    def obs_sum(stage, copies):
        value = so[stage]
        for copy, n in copies:
            copy.wait()
            value = value + so_recv[n]
        return value

    def unpack(k, copies):
        for copy in copies:
            copy.wait()

        def body(l0, _):
            for side, near, far in ((0, 1, 0), (1, 10, 11)):

                def got(n):
                    return hr[k, side, n, lv(l0), :].astype(F32)

                for f in range(5):
                    x[k, f, near, lv(l0), :] = got(f)
                q0[k, near, lv(l0), :] = got(5)
                kt[k, 1, near, lv(l0), :] = got(6)
                ks[k, 1, near, lv(l0), :] = got(7)
                mm[near] = got(8)
                x[k, 0, far, lv(l0), :] = got(9)
                x[k, 1, far, lv(l0), :] = got(10)
                x[k, 2, far, lv(l0), :] = zero
                x[k, 4, far, lv(l0), :] = got(11)
                q0[k, far, lv(l0), :] = got(12)
            return _

        over_chunks(body, 0)

    def tangent(s, q, k, i, l0, m):
        def at(f, n):
            return s[k, f, n, lv(l0), :]

        t, sa, u, v, p = [at(f, i) for f in range(5)]
        qc = q[k, i, lv(l0), :]
        t2 = 0.4 * t + 0.15 * (at(0, i - 1) + at(0, i + 1)) + dn(t) + up(t)
        s2 = 0.4 * sa + 0.15 * (at(1, i - 1) + at(1, i + 1)) + dn(sa) + up(sa)
        u2 = u + r3 * v - 0.15 * (q[k, i + 1, lv(l0), :] - q[k, i - 1, lv(l0), :])
        v2 = v - r3 * u + dn(qc) - up(qc)
        east = at(4, i + 1) - at(2, i + 1)
        west = at(4, i - 1) + at(2, i - 1)
        p2 = 0.4 * p + 0.15 * (east + west) + up(p - v) + dn(p + v)
        return [m * w for w in (t2, s2, u2, v2, p2)]

    def first_substep(k):
        def body(l0, _):
            for i in range(1, 11):
                new = tangent(x, q0, k, i, l0, mm[i])
                for f in range(5):
                    y[k, f, i - 1, lv(l0), :] = new[f]
                q1[k, i - 1, lv(l0), :] = (
                    new[4] + kt[k, 1, i, lv(l0), :] * new[0] + ks[k, 1, i, lv(l0), :] * new[1]
                )
            return _

        over_chunks(body, 0)

    def second_substep(k):
        def body(l0, acc):
            for i in range(1, 9):
                c = i - 1
                m = mm[c + 2]
                new = tangent(y, q1, k, i, l0, m)
                for f in range(5):
                    if k == 1:
                        fw[f, c, lv(l0), :] = new[f]
                        f_send[f, c, lv(l0), :] = new[f].astype(BF16)
                    else:
                        r = r0[1, f, c, lv(l0), :] + new[f]
                        acc = acc + r * r
                        mn = mul_n[5 + f, nat(l0, c), :] + 0.5 * r
                        mn_n[5 + f, nat(l0, c), :] = mn
                        put_edge(0, f, c, l0, m * mn)
            return acc

        macc[...] = over_chunks(body, macc[...])

    def put_edge(k, f, c, l0, w):
        wa[k, f, c + 2, lv(l0), :] = w
        for side, near, far in ((0, 0, 1), (1, 7, 6)):
            if c == near:
                es[k, side, f, lv(l0), :] = w.astype(BF16)
            if c == far and f != 3:
                es[k, side, 5 + (f if f < 3 else 3), lv(l0), :] = w.astype(BF16)

    unpack(1, halo1)
    first_substep(1)
    second_substep(1)
    f_copy = remote(f_send, f_recv, (lax.rem(tm + 1, tm_n), sp))

    @pl.when(tm < tm_n - 1)
    def _():
        f_copy.start()

    unpack(0, halo0)
    first_substep(0)
    second_substep(0)

    def send_edges(k):
        copies = [
            remote(es.at[k, 0], er.at[k, 1], left),
            remote(es.at[k, 1], er.at[k, 0], right),
        ]
        for copy in copies:
            copy.start()
        return copies

    edges0 = send_edges(0)
    outs = []

    def store(src, dst, n):
        copy = pltpu.make_async_copy(src, dst, out_sem.at[n])
        copy.start()
        outs.append(copy)

    store(mn_n.at[part(1)], mn_out.at[part(1)], 1)
    total = sensors(0, total)
    obs1 = obs_stage(0, obs_y)

    @pl.when(tm < tm_n - 1)
    def _():
        b_copy.wait_recv()

    keep = jnp.where(last, 0.0, 1.0)

    def following(l0, _):
        for c in range(8):
            m = keep * mm[c + 2]
            for f in range(5):
                u = b_recv[f, c, lv(l0), :].astype(F32) + 0.5 * fw[f, c, lv(l0), :]
                put_edge(1, f, c, l0, m * u)
        return _

    over_chunks(following, 0)
    edges1 = send_edges(1)

    def transposed(s, k, j, i, col, l0):
        def at(f, n):
            return s[k, f, n, lv(l0), :]

        t, sa, u, v, p = [at(f, i) for f in range(5)]
        pw, pe = at(4, i - 1), at(4, i + 1)
        q = 0.15 * (at(2, i + 1) - at(2, i - 1)) + up(v) - dn(v)
        t2 = 0.4 * t + 0.15 * (at(0, i - 1) + at(0, i + 1)) + dn(t) + up(t)
        t2 = t2 + kt[k, j, col, lv(l0), :] * q
        s2 = 0.4 * sa + 0.15 * (at(1, i - 1) + at(1, i + 1)) + dn(sa) + up(sa)
        s2 = s2 + ks[k, j, col, lv(l0), :] * q
        south, north = dn(p), up(p)
        u2 = u - r3 * v + 0.15 * (pe - pw)
        v2 = v + r3 * u + north - south
        p2 = 0.4 * p + 0.15 * (pe + pw) + south + north + q
        return [t2, s2, u2, v2, p2]

    def first_transposed(k):
        def body(l0, _):
            for i in range(1, 11):
                new = transposed(wa, k, 1, i, i, l0)
                m = mm[i]
                for f in range(5):
                    wb[k, f, i - 1, lv(l0), :] = m * new[f]
            return _

        over_chunks(body, 0)

    def second_transposed(k):
        def body(l0, acc):
            for i in range(1, 9):
                c = i - 1
                new = transposed(wb, k, 0, i, c + 2, l0)
                for f in range(5):
                    if k == 0:
                        rt[f, c, lv(l0), :] = new[f]
                    else:
                        g = mn_n[5 + f, nat(l0, c), :] - new[f]
                        if f < 2:
                            g = g + spread[1, f, nat(l0, c), :]
                        g_n[5 + f, nat(l0, c), :] = g
                        acc = acc + g * g
            return acc

        gacc[...] = over_chunks(body, gacc[...])

    so[1] = obs_sum(0, obs1)
    obs2 = obs_stage(1, obs_z)

    def unpack_edges(k, copies):
        for copy in copies:
            copy.wait()

        def body(l0, _):
            for side, near, far in ((0, 1, 0), (1, 10, 11)):
                for n in range(NEDGE):
                    f = n if n < 5 else (0, 1, 2, 4)[n - 5]
                    i = near if n < 5 else far
                    wa[k, f, i, lv(l0), :] = er[k, side, n, lv(l0), :].astype(F32)
            return _

        over_chunks(body, 0)

    unpack_edges(0, edges0)
    first_transposed(0)
    second_transposed(0)

    so[2] = obs_sum(1, obs2)
    obs3 = obs_stage(2, obs_c)

    unpack_edges(1, edges1)
    first_transposed(1)
    second_transposed(1)

    @pl.when(tm > 0)
    def _():
        f_copy.wait_recv()

    def finish(l0, carry):
        ma, ga = carry
        for f in range(5):
            for c in range(8):
                r = r0[0, f, c, lv(l0), :] + f_recv[f, c, lv(l0), :].astype(F32)
                ma = ma + r * r
                mn = mul_n[f, nat(l0, c), :] + 0.5 * r
                mn_n[f, nat(l0, c), :] = mn
                g = mn - rt[f, c, lv(l0), :]
                if f < 2:
                    g = g + spread[0, f, nat(l0, c), :]
                g_n[f, nat(l0, c), :] = g
                ga = ga + g * g
        return ma, ga

    ma, ga = over_chunks(finish, (macc[...], gacc[...]))
    store(mn_n.at[part(0)], mn_out.at[part(0)], 2)
    ma = jnp.sum(ma, axis=0, keepdims=True) + total[:, :LANES] + total[:, LANES:]
    ga = jnp.sum(ga, axis=0, keepdims=True)
    sub = lax.broadcasted_iota(jnp.int32, (8, LANES), 0)
    value = jnp.where(sub == 0, ma, jnp.where(sub == 1, ga, 0.0))

    pending = []
    n = 0
    for stage, peers in enumerate((group_a, group_b, group_c)):
        ar[stage] = value
        copies = []
        for peer in peers:
            copies.append((remote(ar.at[stage], ar_recv.at[n], peer), n))
            copies[-1][0].start()
            n += 1
        if stage == 0:
            smul = smul_v[...]
            res = inno_v[...] - serr_v[...] * smul - obs_sum(2, obs3)
            sens_n[...] = smul + 0.5 * res
            store(sens_n, sens_out, 0)
        for copy, m in copies:
            copy.wait_recv()
            value = value + ar_recv[m]
        pending += [copy for copy, _ in copies]
    top = jnp.sum(value[0:1], axis=1, keepdims=True)
    below = jnp.sum(value[1:2], axis=1, keepdims=True)
    stride = jnp.broadcast_to(top / (below + 1e-6), (8, LANES))

    pieces = 5
    size = inc_n.shape[0] // pieces

    def update(n, _):
        for r in range(levels):
            at = pl.ds(r * 8, 8)
            g_n[n, at, :] = inc_n[n, at, :] - stride * g_n[n, at, :]
        return _

    for n in range(pieces):
        at = pl.ds(n * size, size)
        lax.fori_loop(n * size, (n + 1) * size, update, 0)
        store(g_n.at[at], inc_out.at[at], 3 + n)

    for copy in pending:
        copy.wait_send()

    @pl.when(tm > 0)
    def _():
        b_copy.wait_send()

    @pl.when(tm < tm_n - 1)
    def _():
        f_copy.wait_send()

    for copy in outs:
        copy.wait()


def on_device(
    dims,
    increment,
    multiplier,
    sensor_multiplier,
    misfit,
    innovation,
    model_error,
    sensor_error,
    trajectory,
    land_sea,
    sensor_cells,
):
    subcount, fields, levels, width, latitude = increment.shape
    rows = levels * width
    nobs = sensor_cells.shape[1]
    zh_n, x_n, y_n, zl_n, c_n = dims
    flat = (subcount * fields, rows, latitude)
    hbm = pl.BlockSpec(memory_space=pltpu.HBM)
    n_obs = (y_n - 1) + (zl_n - 1) + (c_n - 1)
    n_ar = (y_n * c_n - 1) + (x_n - 1) + (zh_n * zl_n - 1)
    n_sem = 10 + n_obs + n_ar

    def v(*shape, dtype=F32):
        return pltpu.VMEM(shape, dtype)

    lr = (levels, latitude)
    increment_next, mult_next, sensor_next = pl.pallas_call(
        functools.partial(main_kernel, dims),
        out_shape=(
            jax.ShapeDtypeStruct(flat, F32),
            jax.ShapeDtypeStruct(flat, F32),
            jax.ShapeDtypeStruct((subcount, nobs), F32),
        ),
        in_specs=[hbm] * 10,
        out_specs=(hbm, hbm, hbm),
        scratch_shapes=[
            v(*flat), v(*flat), v(*flat),
            v(subcount, 2, 2, rows, latitude, dtype=BF16),
            v(*flat), v(*flat), v(subcount, nobs),
            v(width, latitude, dtype=jnp.int32), v(fields, levels),
            v(subcount, nobs, dtype=jnp.int32),
            v(subcount, nobs), v(subcount, nobs), v(subcount, nobs),
            v(fields, *lr),
            v(subcount, 2, rows, latitude),
            v(2 * LANES, 2 * rows, dtype=BF16),
            v(2 * rows, 2 * LANES),
            v(subcount, fields, 12, *lr),
            v(subcount, 2, 12, *lr), v(subcount, 2, 12, *lr),
            v(subcount, 12, *lr),
            v(subcount, fields, 10, *lr),
            v(subcount, 10, *lr),
            v(fields, 8, *lr),
            v(subcount, fields, 8, *lr),
            v(subcount, fields, 12, *lr),
            v(subcount, fields, 10, *lr),
            v(fields, 8, *lr),
            v(12, CH, latitude),
            v(2, 8 * CH, latitude),
            v(subcount, 2, NHALO, *lr, dtype=BF16),
            v(subcount, 2, NHALO, *lr, dtype=BF16),
            v(subcount, 2, NEDGE, *lr, dtype=BF16),
            v(subcount, 2, NEDGE, *lr, dtype=BF16),
            v(fields, 8, *lr, dtype=BF16), v(fields, 8, *lr, dtype=BF16),
            v(fields, 8, *lr, dtype=BF16), v(fields, 8, *lr, dtype=BF16),
            v(CH, latitude), v(CH, latitude),
            v(3, subcount, nobs), v(n_obs, subcount, nobs),
            v(3, 8, latitude), v(n_ar, 8, latitude),
            pltpu.SemaphoreType.DMA((13,)),
            pltpu.SemaphoreType.DMA((8,)),
            pltpu.SemaphoreType.DMA((n_sem,)),
            pltpu.SemaphoreType.DMA((n_sem,)),
        ],
        compiler_params=pltpu.CompilerParams(
            vmem_limit_bytes=67043328, collective_id=0, has_side_effects=True
        ),
        name="uzawa",
    )(
        increment.reshape(flat),
        multiplier.reshape(flat),
        misfit.reshape(flat),
        trajectory.reshape(subcount, 2, 2, rows, latitude),
        land_sea,
        model_error,
        sensor_cells,
        innovation,
        sensor_error,
        sensor_multiplier,
    )
    return (
        increment_next.reshape(increment.shape),
        mult_next.reshape(increment.shape),
        sensor_next,
    )


def solution(mesh, dims=DIMS):
    return jax.shard_map(
        functools.partial(on_device, dims),
        mesh=mesh,
        in_specs=(
            P("tm", None, None, "space", None),
            P("tm", None, None, "space", None),
            P("tm", None),
            P("tm", None, None, "space", None),
            P("tm", None),
            P(),
            P("tm", None),
            P("tm", None, None, None, "space", None),
            P("space", None),
            P("tm", None),
        ),
        out_specs=(
            P("tm", None, None, "space", None),
            P("tm", None, None, "space", None),
            P("tm", None),
        ),
        check_vma=False,
    )
```

```python
import functools

import jax
import jax.numpy as jnp
from jax import lax
from jax.experimental import pallas as pl
from jax.experimental.pallas import tpu as pltpu
from jax.sharding import PartitionSpec as P

MESH = pl.DeviceIdType.MESH
DIMS = (2, 4, 4, 4, 2)
CH = 16
F32 = jnp.float32
BF16 = jnp.bfloat16
NHALO = 13
NEDGE = 9
NRELAY = 2
LANES = 128


def main_kernel(
    dims,
    inc_h, mul_h, mis_h, traj_h, land_h, damp_h, cell_h, inno_h, serr_h, smul_h,
    inc_out, mn_n, sens_n,
    inc_n, mul_n, mis_n, traj_n, g_n,
    land, damp5, cell_v, inno_v, serr_v, smul_v, damp, spread, ft, acc2,
    x, kt, ks, q0, y, q1, fw, r0, wa, wb, rt, mm, kn,
    hs, hr, es, er, f_send, f_recv, b_send, b_recv, relay_buf, macc, gacc,
    so, so_recv, ar, ar_recv,
    in_sem, send_sem, recv_sem,
):
    zh_n, x_n, y_n, zl_n, c_n = dims
    tm = lax.axis_index("tm")
    sp = lax.axis_index("space")
    tm_n = zh_n * x_n
    sp_n = y_n * zl_n * c_n
    zh, xx = tm // x_n, tm % x_n
    yy, zl, cc = sp // (zl_n * c_n), (sp // c_n) % zl_n, sp % c_n
    levels = x.shape[3]
    chunks = levels // CH
    left = (tm, (sp + sp_n - 1) % sp_n)
    right = (tm, (sp + 1) % sp_n)
    first, last = tm == 0, tm == tm_n - 1

    def at_space(dy, dz, dc):
        return (
            ((yy + dy) % y_n) * (zl_n * c_n) + ((zl + dz) % zl_n) * c_n + (cc + dc) % c_n
        )

    group_a = [(tm, at_space(dy, 0, dc)) for dy in range(y_n) for dc in range(c_n) if dy or dc]
    group_b = [(zh * x_n + (xx + dx) % x_n, sp) for dx in range(1, x_n)]
    z_n = zh_n * zl_n
    group_c = []
    for dz in range(1, z_n):
        z = (zh * zl_n + zl + dz) % z_n
        group_c.append(
            ((z // zl_n) * x_n + xx, yy * (zl_n * c_n) + (z % zl_n) * c_n + cc)
        )
    obs_y = [(tm, at_space(dy, 0, 0)) for dy in range(1, y_n)]
    obs_z = [(tm, at_space(0, dz, 0)) for dz in range(1, zl_n)]
    obs_c = [(tm, at_space(0, 0, dc)) for dc in range(1, c_n)]

    loads = {}

    def load(name, src, dst, n):
        copy = pltpu.make_async_copy(src, dst, in_sem.at[n])
        copy.start()
        loads[name] = copy

    n_in = inc_n.shape[0] // 2

    def part(k):
        return pl.ds(k * n_in, n_in)

    load("inc1", inc_h.at[part(1)], inc_n.at[part(1)], 0)
    load("traj", traj_h, traj_n, 1)
    load("land", land_h, land, 2)
    load("damp", damp_h, damp5, 3)
    load("inc0", inc_h.at[part(0)], inc_n.at[part(0)], 4)
    load("mul0", mul_h.at[part(0)], mul_n.at[part(0)], 5)
    load("mis0", mis_h.at[part(0)], mis_n.at[part(0)], 6)
    load("cell", cell_h, cell_v, 7)
    load("inno", inno_h, inno_v, 8)
    load("serr", serr_h, serr_v, 9)
    load("smul", smul_h, smul_v, 10)
    load("mul1", mul_h.at[part(1)], mul_n.at[part(1)], 11)
    load("mis1", mis_h.at[part(1)], mis_n.at[part(1)], 12)

    barrier = pltpu.get_barrier_semaphore()
    everyone = [left, right] + group_a + group_b + group_c + obs_y + obs_z + obs_c
    for peer in everyone:
        pl.semaphore_signal(barrier, inc=1, device_id=peer, device_id_type=MESH)

    @pl.when(tm > 0)
    def _():
        pl.semaphore_signal(barrier, inc=1, device_id=(tm - 1, sp), device_id_type=MESH)

    @pl.when(tm < tm_n - 1)
    def _():
        pl.semaphore_signal(barrier, inc=1, device_id=(tm + 1, sp), device_id_type=MESH)

    sem_n = [0]

    def remote(src, dst, peer, arrives=None):
        n = sem_n[0]
        sem_n[0] += 1
        arrives = n if arrives is None else arrives
        return pltpu.make_async_remote_copy(
            src_ref=src, dst_ref=dst, send_sem=send_sem.at[n], recv_sem=recv_sem.at[arrives],
            device_id=peer, device_id_type=MESH,
        )

    class Shift:
        def __init__(self, src, dst, by):
            goal = (lax.rem(tm + by + tm_n, tm_n), sp)
            start_x, end_x = (x_n - 1, 0) if by == 1 else (0, x_n - 1)
            start_z, end_z = (zh < zh_n - 1, zh > 0) if by == 1 else (zh > 0, zh < zh_n - 1)
            self.sends = tm < tm_n - 1 if by == 1 else tm > 0
            self.gets = tm > 0 if by == 1 else tm < tm_n - 1
            self.crosses = (xx == start_x) & start_z
            self.relays = (xx == end_x) & start_z
            relay = (zh * x_n + end_x, sp)
            other = (lax.rem(tm + by * x_n + tm_n, tm_n), sp)
            self.whole = remote(src.at[NRELAY:], dst.at[NRELAY:], goal)
            self.direct, self.leg1, self.leg2 = [], [], []
            for f in range(NRELAY):
                n = sem_n[0]
                self.direct.append(remote(src.at[f], dst.at[f], goal))
                self.leg1.append(remote(src.at[f], relay_buf.at[f], relay))
                self.leg2.append(remote(relay_buf.at[f], dst.at[f], other, arrives=n))

        def start(self):
            @pl.when(self.crosses)
            def _():
                for copy in self.leg1:
                    copy.start()

            @pl.when(self.sends)
            def _():
                self.whole.start()

            @pl.when(self.sends & jnp.logical_not(self.crosses))
            def _():
                for copy in self.direct:
                    copy.start()

        def hand_on(self):
            @pl.when(self.relays)
            def _():
                for one, two in zip(self.leg1, self.leg2):
                    one.wait_recv()
                    two.start()

        def wait_recv(self):
            @pl.when(self.gets)
            def _():
                self.whole.wait_recv()
                for copy in self.direct:
                    copy.wait_recv()

        def wait_send(self):
            @pl.when(self.crosses)
            def _():
                for copy in self.leg1:
                    copy.wait_send()

            @pl.when(self.sends)
            def _():
                self.whole.wait_send()

            @pl.when(self.sends & jnp.logical_not(self.crosses))
            def _():
                for copy in self.direct:
                    copy.wait_send()

            @pl.when(self.relays)
            def _():
                for copy in self.leg2:
                    copy.wait_send()

    lane = lax.broadcasted_iota(jnp.int32, (CH, LANES), 1)
    c_dn = jnp.where(lane > 0, 0.15, 0.0)
    c_up = jnp.where(lane < LANES - 1, 0.15, 0.0)
    r3 = (0.3 * 0.5 / (0.5 * LANES)) * (lane.astype(F32) - 0.5 * (LANES - 1))

    def dn(v):
        return c_dn * pltpu.roll(v, 1, 1)

    def up(v):
        return c_up * pltpu.roll(v, LANES - 1, 1)

    def over_chunks(body, init=None):
        def step(n, carry):
            return body(pl.multiple_of(n * CH, CH), carry)

        return lax.fori_loop(0, chunks, step, init)

    def nat(l0, c):
        return pl.ds(l0 * 8 + c, CH, stride=8)

    def lv(l0):
        return pl.ds(l0, CH)

    zero = jnp.zeros((CH, LANES), F32)
    macc[...] = zero
    gacc[...] = zero

    def constants():
        for c in range(8):
            mm[c + 2] = jnp.broadcast_to(land[c : c + 1, :].astype(F32), (CH, LANES))
        same = lax.broadcasted_iota(jnp.int32, (levels, levels), 0) == (
            lax.broadcasted_iota(jnp.int32, (levels, levels), 1)
        )
        for f in range(5):
            spot = jnp.where(same, damp5[f : f + 1, :], 0.0)
            damp[f] = jnp.broadcast_to(jnp.sum(spot, axis=1, keepdims=True), (levels, LANES))

    def residual(k, with_send):
        def body(l0, _):
            for f in range(5):
                d = damp[f, lv(l0), :]
                for c in range(8):
                    mu = mul_n[k * 5 + f, nat(l0, c), :]
                    v = inc_n[k * 5 + f, nat(l0, c), :]
                    r = mis_n[k * 5 + f, nat(l0, c), :] - d * mu - v
                    r0[k, f, c, lv(l0), :] = r
                    if with_send:
                        b_send[f, c, lv(l0), :] = (mu + 0.5 * r).astype(BF16)
            return _

        over_chunks(body, 0)

    def prepare(k):
        def body(l0, _):
            for j in range(2):
                h0 = traj_n[k, j, 0, pl.ds(l0 * 8, 8 * CH), :].astype(F32)
                h1 = traj_n[k, j, 1, pl.ds(l0 * 8, 8 * CH), :].astype(F32)
                kn[0] = -0.6 * h0 + 0.08 * h1 - 0.05
                kn[1] = 0.7 + 0.3 * h0
                for c in range(8):
                    kt[k, j, c + 2, lv(l0), :] = kn[0, pl.ds(c, CH, stride=8), :]
                    ks[k, j, c + 2, lv(l0), :] = kn[1, pl.ds(c, CH, stride=8), :]
            for c in range(8):
                v = [inc_n[k * 5 + f, nat(l0, c), :] for f in range(5)]
                for f in range(5):
                    x[k, f, c + 2, lv(l0), :] = v[f]
                q = (
                    v[4]
                    + kt[k, 0, c + 2, lv(l0), :] * v[0]
                    + ks[k, 0, c + 2, lv(l0), :] * v[1]
                )
                q0[k, c + 2, lv(l0), :] = q
                for side, near, far in ((0, 0, 1), (1, 7, 6)):
                    out = []
                    if c == near:
                        out = list(enumerate(v + [q])) + [
                            (6, kt[k, 1, c + 2, lv(l0), :]),
                            (7, ks[k, 1, c + 2, lv(l0), :]),
                            (8, mm[c + 2]),
                        ]
                    if c == far:
                        pu = v[4] - v[2] if side == 0 else v[4] + v[2]
                        out = [(9, v[0]), (10, v[1]), (11, pu), (12, q)]
                    for n, value in out:
                        hs[k, side, n, lv(l0), :] = value.astype(BF16)
            return _

        over_chunks(body, 0)

    def send_halo(k):
        copies = [
            remote(hs.at[k, 0], hr.at[k, 1], left),
            remote(hs.at[k, 1], hr.at[k, 0], right),
        ]
        for copy in copies:
            copy.start()
        return copies

    for name in ("inc1", "traj", "land", "damp"):
        loads[name].wait()
    constants()
    prepare(1)
    for name in ("inc0", "mul0", "mis0"):
        loads[name].wait()
    residual(0, True)

    n_edge = jnp.where(first, 0, 1) + jnp.where(last, 0, 1)
    pl.semaphore_wait(barrier, len(everyone) + n_edge)
    halo1 = send_halo(1)

    b_copy = Shift(b_send, b_recv, -1)
    b_copy.start()

    @pl.when(last)
    def _():
        b_recv[...] = jnp.zeros_like(b_recv)

    @pl.when(first)
    def _():
        f_recv[...] = jnp.zeros_like(f_recv)

    prepare(0)
    halo0 = send_halo(0)

    subcount, nobs = cell_v.shape
    rows = ft.shape[1]
    block = 256
    columns = 8 * sp_n
    offset = sp * 8
    row_id = lax.broadcasted_iota(jnp.int32, (rows, block), 0)
    lane_id = lax.broadcasted_iota(jnp.int32, (LANES, block), 0)

    def sensors(k, total):
        turned = inc_n[k * 5 : k * 5 + 2].reshape(rows, LANES).T
        high = turned.astype(BF16)
        ft[0:LANES, :] = high
        ft[LANES:, :] = (turned - high.astype(F32)).astype(BF16)
        acc2[...] = jnp.zeros_like(acc2)

        def chunk(n, total):
            at = pl.ds(pl.multiple_of(n * block, block), block)
            cell = cell_v[k : k + 1, at]
            row = cell & (LANES - 1)
            rest = cell >> 7
            col = rest & (columns - 1)
            level = rest >> (columns.bit_length() - 1)
            own = (col >= offset) & (col < offset + 8)
            local = jnp.where(own, level * 8 + col - offset, -1)
            hot = jnp.where(row_id == local, 1.0, 0.0).astype(BF16)
            on_lane = lane_id == row
            picked = jnp.dot(ft[...], hot, preferred_element_type=F32)
            both = picked[:LANES] + picked[LANES:]
            obs = jnp.sum(jnp.where(on_lane, both, 0.0), axis=0, keepdims=True)
            smul = smul_v[k : k + 1, at]
            res = inno_v[k : k + 1, at] - serr_v[k : k + 1, at] * smul - obs
            put = jnp.where(on_lane, smul + 0.5 * res, 0.0)
            put_high = put.astype(BF16)
            put_low = (put - put_high.astype(F32)).astype(BF16)
            put2 = jnp.concatenate([put_high, put_low], axis=0)
            acc2[...] += lax.dot_general(
                hot, put2, (((1,), (1,)), ((), ())), preferred_element_type=F32
            )
            so[0, k : k + 1, at] = obs
            return total + jnp.where(own, res * res, 0.0)

        total = lax.fori_loop(0, nobs // block, chunk, total)
        both = acc2[:, :LANES] + acc2[:, LANES:]
        spread[k] = both.reshape(spread.shape[1:])
        return total

    for name in ("cell", "inno", "serr", "smul", "mul1", "mis1"):
        loads[name].wait()
    residual(1, False)
    b_copy.hand_on()
    total = sensors(1, jnp.zeros((1, block), F32))

    slot = [0]

    def obs_stage(stage, peers):
        copies = []
        for peer in peers:
            copies.append((remote(so.at[stage], so_recv.at[slot[0]], peer), slot[0]))
            copies[-1][0].start()
            slot[0] += 1
        return copies

    def obs_sum(stage, copies):
        value = so[stage]
        for copy, n in copies:
            copy.wait()
            value = value + so_recv[n]
        return value

    def unpack(k, copies):
        for copy in copies:
            copy.wait()

        def body(l0, _):
            for side, near, far in ((0, 1, 0), (1, 10, 11)):

                def got(n):
                    return hr[k, side, n, lv(l0), :].astype(F32)

                for f in range(5):
                    x[k, f, near, lv(l0), :] = got(f)
                q0[k, near, lv(l0), :] = got(5)
                kt[k, 1, near, lv(l0), :] = got(6)
                ks[k, 1, near, lv(l0), :] = got(7)
                mm[near] = got(8)
                x[k, 0, far, lv(l0), :] = got(9)
                x[k, 1, far, lv(l0), :] = got(10)
                x[k, 2, far, lv(l0), :] = zero
                x[k, 4, far, lv(l0), :] = got(11)
                q0[k, far, lv(l0), :] = got(12)
            return _

        over_chunks(body, 0)

    def tangent(s, q, k, i, l0, m):
        def at(f, n):
            return s[k, f, n, lv(l0), :]

        t, sa, u, v, p = [at(f, i) for f in range(5)]
        qc = q[k, i, lv(l0), :]
        t2 = 0.4 * t + 0.15 * (at(0, i - 1) + at(0, i + 1)) + dn(t) + up(t)
        s2 = 0.4 * sa + 0.15 * (at(1, i - 1) + at(1, i + 1)) + dn(sa) + up(sa)
        u2 = u + r3 * v - 0.15 * (q[k, i + 1, lv(l0), :] - q[k, i - 1, lv(l0), :])
        v2 = v - r3 * u + dn(qc) - up(qc)
        east = at(4, i + 1) - at(2, i + 1)
        west = at(4, i - 1) + at(2, i - 1)
        p2 = 0.4 * p + 0.15 * (east + west) + up(p - v) + dn(p + v)
        return [m * w for w in (t2, s2, u2, v2, p2)]

    def first_substep(k):
        def body(l0, _):
            for i in range(1, 11):
                new = tangent(x, q0, k, i, l0, mm[i])
                for f in range(5):
                    y[k, f, i - 1, lv(l0), :] = new[f]
                q1[k, i - 1, lv(l0), :] = (
                    new[4] + kt[k, 1, i, lv(l0), :] * new[0] + ks[k, 1, i, lv(l0), :] * new[1]
                )
            return _

        over_chunks(body, 0)

    def second_substep(k):
        def body(l0, acc):
            for i in range(1, 9):
                c = i - 1
                m = mm[c + 2]
                new = tangent(y, q1, k, i, l0, m)
                for f in range(5):
                    if k == 1:
                        fw[f, c, lv(l0), :] = new[f]
                        f_send[f, c, lv(l0), :] = new[f].astype(BF16)
                    else:
                        r = r0[1, f, c, lv(l0), :] + new[f]
                        acc = acc + r * r
                        mn = mul_n[5 + f, nat(l0, c), :] + 0.5 * r
                        mn_n[5 + f, nat(l0, c), :] = mn
                        put_edge(0, f, c, l0, m * mn)
            return acc

        macc[...] = over_chunks(body, macc[...])

    def put_edge(k, f, c, l0, w):
        wa[k, f, c + 2, lv(l0), :] = w
        for side, near, far in ((0, 0, 1), (1, 7, 6)):
            if c == near:
                es[k, side, f, lv(l0), :] = w.astype(BF16)
            if c == far and f != 3:
                es[k, side, 5 + (f if f < 3 else 3), lv(l0), :] = w.astype(BF16)

    unpack(1, halo1)
    first_substep(1)
    second_substep(1)
    f_copy = Shift(f_send, f_recv, 1)
    f_copy.start()

    unpack(0, halo0)
    first_substep(0)
    second_substep(0)

    def send_edges(k):
        copies = [
            remote(es.at[k, 0], er.at[k, 1], left),
            remote(es.at[k, 1], er.at[k, 0], right),
        ]
        for copy in copies:
            copy.start()
        return copies

    edges0 = send_edges(0)
    f_copy.hand_on()
    outs = []

    def store(src, dst, n):
        copy = pltpu.make_async_copy(src, dst, out_sem.at[n])
        copy.start()
        outs.append(copy)

    total = sensors(0, total)
    obs1 = obs_stage(0, obs_y)

    b_copy.wait_recv()

    keep = jnp.where(last, 0.0, 1.0)

    def following(l0, _):
        for c in range(8):
            m = keep * mm[c + 2]
            for f in range(5):
                u = b_recv[f, c, lv(l0), :].astype(F32) + 0.5 * fw[f, c, lv(l0), :]
                put_edge(1, f, c, l0, m * u)
        return _

    over_chunks(following, 0)
    edges1 = send_edges(1)

    def transposed(s, k, j, i, col, l0):
        def at(f, n):
            return s[k, f, n, lv(l0), :]

        t, sa, u, v, p = [at(f, i) for f in range(5)]
        pw, pe = at(4, i - 1), at(4, i + 1)
        q = 0.15 * (at(2, i + 1) - at(2, i - 1)) + up(v) - dn(v)
        t2 = 0.4 * t + 0.15 * (at(0, i - 1) + at(0, i + 1)) + dn(t) + up(t)
        t2 = t2 + kt[k, j, col, lv(l0), :] * q
        s2 = 0.4 * sa + 0.15 * (at(1, i - 1) + at(1, i + 1)) + dn(sa) + up(sa)
        s2 = s2 + ks[k, j, col, lv(l0), :] * q
        south, north = dn(p), up(p)
        u2 = u - r3 * v + 0.15 * (pe - pw)
        v2 = v + r3 * u + north - south
        p2 = 0.4 * p + 0.15 * (pe + pw) + south + north + q
        return [t2, s2, u2, v2, p2]

    def first_transposed(k):
        def body(l0, _):
            for i in range(1, 11):
                new = transposed(wa, k, 1, i, i, l0)
                m = mm[i]
                for f in range(5):
                    wb[k, f, i - 1, lv(l0), :] = m * new[f]
            return _

        over_chunks(body, 0)

    def second_transposed(k):
        def body(l0, acc):
            for i in range(1, 9):
                c = i - 1
                new = transposed(wb, k, 0, i, c + 2, l0)
                for f in range(5):
                    if k == 0:
                        rt[f, c, lv(l0), :] = new[f]
                    else:
                        g = mn_n[5 + f, nat(l0, c), :] - new[f]
                        if f < 2:
                            g = g + spread[1, f, nat(l0, c), :]
                        g_n[5 + f, nat(l0, c), :] = g
                        acc = acc + g * g
            return acc

        gacc[...] = over_chunks(body, gacc[...])

    so[1] = obs_sum(0, obs1)
    obs2 = obs_stage(1, obs_z)

    def unpack_edges(k, copies):
        for copy in copies:
            copy.wait()

        def body(l0, _):
            for side, near, far in ((0, 1, 0), (1, 10, 11)):
                for n in range(NEDGE):
                    f = n if n < 5 else (0, 1, 2, 4)[n - 5]
                    i = near if n < 5 else far
                    wa[k, f, i, lv(l0), :] = er[k, side, n, lv(l0), :].astype(F32)
            return _

        over_chunks(body, 0)

    unpack_edges(0, edges0)
    first_transposed(0)
    second_transposed(0)

    so[2] = obs_sum(1, obs2)
    obs3 = obs_stage(2, obs_c)

    unpack_edges(1, edges1)
    first_transposed(1)
    second_transposed(1)

    f_copy.wait_recv()

    def finish(l0, carry):
        ma, ga = carry
        for f in range(5):
            for c in range(8):
                r = r0[0, f, c, lv(l0), :] + f_recv[f, c, lv(l0), :].astype(F32)
                ma = ma + r * r
                mn = mul_n[f, nat(l0, c), :] + 0.5 * r
                mn_n[f, nat(l0, c), :] = mn
                g = mn - rt[f, c, lv(l0), :]
                if f < 2:
                    g = g + spread[0, f, nat(l0, c), :]
                g_n[f, nat(l0, c), :] = g
                ga = ga + g * g
        return ma, ga

    ma, ga = over_chunks(finish, (macc[...], gacc[...]))
    ma = jnp.sum(ma, axis=0, keepdims=True) + total[:, :LANES] + total[:, LANES:]
    ga = jnp.sum(ga, axis=0, keepdims=True)
    sub = lax.broadcasted_iota(jnp.int32, (8, LANES), 0)
    value = jnp.where(sub == 0, ma, jnp.where(sub == 1, ga, 0.0))

    pending = []
    n = 0
    for stage, peers in enumerate((group_a, group_b, group_c)):
        ar[stage] = value
        copies = []
        for peer in peers:
            copies.append((remote(ar.at[stage], ar_recv.at[n], peer), n))
            copies[-1][0].start()
            n += 1
        if stage == 0:
            smul = smul_v[...]
            res = inno_v[...] - serr_v[...] * smul - obs_sum(2, obs3)
            sens_n[...] = smul + 0.5 * res
        for copy, m in copies:
            copy.wait_recv()
            value = value + ar_recv[m]
        pending += [copy for copy, _ in copies]
    top = jnp.sum(value[0:1], axis=1, keepdims=True)
    below = jnp.sum(value[1:2], axis=1, keepdims=True)
    stride = jnp.broadcast_to(top / (below + 1e-6), (8, LANES))

    pieces = 5
    size = inc_n.shape[0] // pieces

    def update(n, _):
        for r in range(levels):
            at = pl.ds(r * 8, 8)
            inc_out[n, at, :] = inc_n[n, at, :] - stride * g_n[n, at, :]
        return _

    for n in range(pieces):
        at = pl.ds(n * size, size)
        lax.fori_loop(n * size, (n + 1) * size, update, 0)

    for copy in pending:
        copy.wait_send()

    b_copy.wait_send()
    f_copy.wait_send()

    for copy in outs:
        copy.wait()


def on_device(
    dims,
    increment,
    multiplier,
    sensor_multiplier,
    misfit,
    innovation,
    model_error,
    sensor_error,
    trajectory,
    land_sea,
    sensor_cells,
):
    subcount, fields, levels, width, latitude = increment.shape
    rows = levels * width
    nobs = sensor_cells.shape[1]
    zh_n, x_n, y_n, zl_n, c_n = dims
    flat = (subcount * fields, rows, latitude)
    vm = pl.BlockSpec(memory_space=pltpu.VMEM)
    hbm = pl.BlockSpec(memory_space=pltpu.HBM)
    n_obs = (y_n - 1) + (zl_n - 1) + (c_n - 1)
    n_ar = (y_n * c_n - 1) + (x_n - 1) + (zh_n * zl_n - 1)
    n_sem = 10 + 6 * NRELAY + n_obs + n_ar

    def v(*shape, dtype=F32):
        return pltpu.VMEM(shape, dtype)

    lr = (levels, latitude)
    increment_next, mult_next, sensor_next = pl.pallas_call(
        functools.partial(main_kernel, dims),
        out_shape=(
            jax.ShapeDtypeStruct(flat, F32),
            jax.ShapeDtypeStruct(flat, F32),
            jax.ShapeDtypeStruct((subcount, nobs), F32),
        ),
        in_specs=[hbm] * 10,
        out_specs=(vm, vm, vm),
        scratch_shapes=[
            v(*flat), v(*flat), v(*flat),
            v(subcount, 2, 2, rows, latitude, dtype=BF16),
            v(*flat),
            v(width, latitude, dtype=jnp.int32), v(fields, levels),
            v(subcount, nobs, dtype=jnp.int32),
            v(subcount, nobs), v(subcount, nobs), v(subcount, nobs),
            v(fields, *lr),
            v(subcount, 2, rows, latitude),
            v(2 * LANES, 2 * rows, dtype=BF16),
            v(2 * rows, 2 * LANES),
            v(subcount, fields, 12, *lr),
            v(subcount, 2, 12, *lr), v(subcount, 2, 12, *lr),
            v(subcount, 12, *lr),
            v(subcount, fields, 10, *lr),
            v(subcount, 10, *lr),
            v(fields, 8, *lr),
            v(subcount, fields, 8, *lr),
            v(subcount, fields, 12, *lr),
            v(subcount, fields, 10, *lr),
            v(fields, 8, *lr),
            v(12, CH, latitude),
            v(2, 8 * CH, latitude),
            v(subcount, 2, NHALO, *lr, dtype=BF16),
            v(subcount, 2, NHALO, *lr, dtype=BF16),
            v(subcount, 2, NEDGE, *lr, dtype=BF16),
            v(subcount, 2, NEDGE, *lr, dtype=BF16),
            v(fields, 8, *lr, dtype=BF16), v(fields, 8, *lr, dtype=BF16),
            v(fields, 8, *lr, dtype=BF16), v(fields, 8, *lr, dtype=BF16),
            v(NRELAY, 8, *lr, dtype=BF16),
            v(CH, latitude), v(CH, latitude),
            v(3, subcount, nobs), v(n_obs, subcount, nobs),
            v(3, 8, latitude), v(n_ar, 8, latitude),
            pltpu.SemaphoreType.DMA((13,)),
            pltpu.SemaphoreType.DMA((n_sem,)),
            pltpu.SemaphoreType.DMA((n_sem,)),
        ],
        compiler_params=pltpu.CompilerParams(
            vmem_limit_bytes=46 << 20, collective_id=0, has_side_effects=True
        ),
        name="uzawa",
    )(*[pltpu.with_memory_space_constraint(a, pltpu.HBM) for a in (
        increment.reshape(flat),
        multiplier.reshape(flat),
        misfit.reshape(flat),
        trajectory.reshape(subcount, 2, 2, rows, latitude),
        land_sea,
        model_error,
        sensor_cells,
        innovation,
        sensor_error,
        sensor_multiplier,
    )])
    return (
        increment_next.reshape(increment.shape),
        mult_next.reshape(increment.shape),
        sensor_next,
    )


def solution(mesh, dims=DIMS):
    return jax.shard_map(
        functools.partial(on_device, dims),
        mesh=mesh,
        in_specs=(
            P("tm", None, None, "space", None),
            P("tm", None, None, "space", None),
            P("tm", None),
            P("tm", None, None, "space", None),
            P("tm", None),
            P(),
            P("tm", None),
            P("tm", None, None, None, "space", None),
            P("space", None),
            P("tm", None),
        ),
        out_specs=(
            P("tm", None, None, "space", None),
            P("tm", None, None, "space", None),
            P("tm", None),
        ),
        check_vma=False,
    )
```

```python
import functools

import jax
import jax.numpy as jnp
from jax import lax
from jax.experimental import pallas as pl
from jax.experimental.pallas import tpu as pltpu
from jax.sharding import PartitionSpec as P

MESH = pl.DeviceIdType.MESH
DIMS = (2, 4, 4, 4, 2)
CH = 16
F32 = jnp.float32
BF16 = jnp.bfloat16
NHALO = 13
NEDGE = 9
NRELAY = 2
LANES = 128


def main_kernel(
    dims,
    inc_h, mul_h, mis_h, traj_h, land_h, damp_h, cell_h, inno_h, serr_h, smul_h,
    inc_out, mn_n, sens_n,
    inc_n, mul_n, mis_n, traj_n, g_n,
    land, damp5, cell_v, inno_v, serr_v, smul_v, damp, spread, ft, acc2,
    x, kt, ks, q0, y, q1, fw, r0, wa, wb, rt, mm, kn,
    hs, hr, es, er, f_send, f_recv, b_send, b_recv, relay_buf, macc, gacc,
    so, so_recv, ar, ar_recv,
    in_sem, send_sem, recv_sem,
):
    zh_n, x_n, y_n, zl_n, c_n = dims
    tm = lax.axis_index("tm")
    sp = lax.axis_index("space")
    tm_n = zh_n * x_n
    sp_n = y_n * zl_n * c_n
    zh, xx = tm // x_n, tm % x_n
    yy, zl, cc = sp // (zl_n * c_n), (sp // c_n) % zl_n, sp % c_n
    levels = x.shape[3]
    chunks = levels // CH
    left = (tm, (sp + sp_n - 1) % sp_n)
    right = (tm, (sp + 1) % sp_n)
    first, last = tm == 0, tm == tm_n - 1

    def at_space(dy, dz, dc):
        return (
            ((yy + dy) % y_n) * (zl_n * c_n) + ((zl + dz) % zl_n) * c_n + (cc + dc) % c_n
        )

    group_a = [(tm, at_space(dy, 0, dc)) for dy in range(y_n) for dc in range(c_n) if dy or dc]
    group_b = [(zh * x_n + (xx + dx) % x_n, sp) for dx in range(1, x_n)]
    z_n = zh_n * zl_n
    group_c = []
    for dz in range(1, z_n):
        z = (zh * zl_n + zl + dz) % z_n
        group_c.append(
            ((z // zl_n) * x_n + xx, yy * (zl_n * c_n) + (z % zl_n) * c_n + cc)
        )
    obs_y = [(tm, at_space(dy, 0, 0)) for dy in range(1, y_n)]
    obs_z = [(tm, at_space(0, dz, 0)) for dz in range(1, zl_n)]
    obs_c = [(tm, at_space(0, 0, dc)) for dc in range(1, c_n)]

    loads = {}

    def load(name, src, dst, n):
        copy = pltpu.make_async_copy(src, dst, in_sem.at[n])
        copy.start()
        loads[name] = copy

    n_in = inc_n.shape[0] // 2

    def part(k):
        return pl.ds(k * n_in, n_in)

    load("inc1", inc_h.at[part(1)], inc_n.at[part(1)], 0)
    load("traj", traj_h, traj_n, 1)
    load("land", land_h, land, 2)
    load("damp", damp_h, damp5, 3)
    load("inc0", inc_h.at[part(0)], inc_n.at[part(0)], 4)
    load("mul0", mul_h.at[part(0)], mul_n.at[part(0)], 5)
    load("mis0", mis_h.at[part(0)], mis_n.at[part(0)], 6)
    load("cell", cell_h, cell_v, 7)
    load("inno", inno_h, inno_v, 8)
    load("serr", serr_h, serr_v, 9)
    load("smul", smul_h, smul_v, 10)
    load("mul1", mul_h.at[part(1)], mul_n.at[part(1)], 11)
    load("mis1", mis_h.at[part(1)], mis_n.at[part(1)], 12)

    barrier = pltpu.get_barrier_semaphore()
    everyone = [left, right] + group_a + group_b + group_c + obs_y + obs_z + obs_c
    for peer in everyone:
        pl.semaphore_signal(barrier, inc=1, device_id=peer, device_id_type=MESH)

    @pl.when(tm > 0)
    def _():
        pl.semaphore_signal(barrier, inc=1, device_id=(tm - 1, sp), device_id_type=MESH)

    @pl.when(tm < tm_n - 1)
    def _():
        pl.semaphore_signal(barrier, inc=1, device_id=(tm + 1, sp), device_id_type=MESH)

    sem_n = [0]

    def remote(src, dst, peer, arrives=None):
        n = sem_n[0]
        sem_n[0] += 1
        arrives = n if arrives is None else arrives
        return pltpu.make_async_remote_copy(
            src_ref=src, dst_ref=dst, send_sem=send_sem.at[n], recv_sem=recv_sem.at[arrives],
            device_id=peer, device_id_type=MESH,
        )

    class Shift:
        def __init__(self, src, dst, by):
            goal = (lax.rem(tm + by + tm_n, tm_n), sp)
            start_x, end_x = (x_n - 1, 0) if by == 1 else (0, x_n - 1)
            start_z, end_z = (zh < zh_n - 1, zh > 0) if by == 1 else (zh > 0, zh < zh_n - 1)
            self.sends = tm < tm_n - 1 if by == 1 else tm > 0
            self.gets = tm > 0 if by == 1 else tm < tm_n - 1
            self.crosses = (xx == start_x) & start_z
            self.relays = (xx == end_x) & start_z
            relay = (zh * x_n + end_x, sp)
            other = (lax.rem(tm + by * x_n + tm_n, tm_n), sp)
            self.whole = remote(src.at[NRELAY:], dst.at[NRELAY:], goal)
            self.direct, self.leg1, self.leg2 = [], [], []
            for f in range(NRELAY):
                n = sem_n[0]
                self.direct.append(remote(src.at[f], dst.at[f], goal))
                self.leg1.append(remote(src.at[f], relay_buf.at[f], relay))
                self.leg2.append(remote(relay_buf.at[f], dst.at[f], other, arrives=n))

        def start(self):
            @pl.when(self.crosses)
            def _():
                for copy in self.leg1:
                    copy.start()

            @pl.when(self.sends)
            def _():
                self.whole.start()

            @pl.when(self.sends & jnp.logical_not(self.crosses))
            def _():
                for copy in self.direct:
                    copy.start()

        def hand_on(self):
            @pl.when(self.relays)
            def _():
                for one, two in zip(self.leg1, self.leg2):
                    one.wait_recv()
                    two.start()

        def wait_recv(self):
            @pl.when(self.gets)
            def _():
                self.whole.wait_recv()
                for copy in self.direct:
                    copy.wait_recv()

        def wait_send(self):
            @pl.when(self.crosses)
            def _():
                for copy in self.leg1:
                    copy.wait_send()

            @pl.when(self.sends)
            def _():
                self.whole.wait_send()

            @pl.when(self.sends & jnp.logical_not(self.crosses))
            def _():
                for copy in self.direct:
                    copy.wait_send()

            @pl.when(self.relays)
            def _():
                for copy in self.leg2:
                    copy.wait_send()

    lane = lax.broadcasted_iota(jnp.int32, (CH, LANES), 1)
    c_dn = jnp.where(lane > 0, 0.15, 0.0)
    c_up = jnp.where(lane < LANES - 1, 0.15, 0.0)
    r3 = (0.3 * 0.5 / (0.5 * LANES)) * (lane.astype(F32) - 0.5 * (LANES - 1))

    def dn(v):
        return c_dn * pltpu.roll(v, 1, 1)

    def up(v):
        return c_up * pltpu.roll(v, LANES - 1, 1)

    def over_chunks(body, init=None):
        def step(n, carry):
            return body(pl.multiple_of(n * CH, CH), carry)

        return lax.fori_loop(0, chunks, step, init)

    def nat(l0, c):
        return pl.ds(l0 * 8 + c, CH, stride=8)

    def lv(l0):
        return pl.ds(l0, CH)

    zero = jnp.zeros((CH, LANES), F32)
    macc[...] = zero
    gacc[...] = zero

    def constants():
        for c in range(8):
            mm[c + 2] = jnp.broadcast_to(land[c : c + 1, :].astype(F32), (CH, LANES))
        same = lax.broadcasted_iota(jnp.int32, (levels, levels), 0) == (
            lax.broadcasted_iota(jnp.int32, (levels, levels), 1)
        )
        for f in range(5):
            spot = jnp.where(same, damp5[f : f + 1, :], 0.0)
            damp[f] = jnp.broadcast_to(jnp.sum(spot, axis=1, keepdims=True), (levels, LANES))

    def residual(k, with_send):
        def body(l0, _):
            for f in range(5):
                d = damp[f, lv(l0), :]
                for c in range(8):
                    mu = mul_n[k * 5 + f, nat(l0, c), :]
                    v = inc_n[k * 5 + f, nat(l0, c), :]
                    r = mis_n[k * 5 + f, nat(l0, c), :] - d * mu - v
                    r0[k, f, c, lv(l0), :] = r
                    if with_send:
                        b_send[f, c, lv(l0), :] = (mu + 0.5 * r).astype(BF16)
            return _

        over_chunks(body, 0)

    def prepare(k):
        def body(l0, _):
            for j in range(2):
                h0 = traj_n[k, j, 0, pl.ds(l0 * 8, 8 * CH), :].astype(F32)
                h1 = traj_n[k, j, 1, pl.ds(l0 * 8, 8 * CH), :].astype(F32)
                kn[0] = -0.6 * h0 + 0.08 * h1 - 0.05
                kn[1] = 0.7 + 0.3 * h0
                for c in range(8):
                    kt[k, j, c + 2, lv(l0), :] = kn[0, pl.ds(c, CH, stride=8), :]
                    ks[k, j, c + 2, lv(l0), :] = kn[1, pl.ds(c, CH, stride=8), :]
            for c in range(8):
                v = [inc_n[k * 5 + f, nat(l0, c), :] for f in range(5)]
                for f in range(5):
                    x[k, f, c + 2, lv(l0), :] = v[f]
                q = (
                    v[4]
                    + kt[k, 0, c + 2, lv(l0), :] * v[0]
                    + ks[k, 0, c + 2, lv(l0), :] * v[1]
                )
                q0[k, c + 2, lv(l0), :] = q
                for side, near, far in ((0, 0, 1), (1, 7, 6)):
                    out = []
                    if c == near:
                        out = list(enumerate(v + [q])) + [
                            (6, kt[k, 1, c + 2, lv(l0), :]),
                            (7, ks[k, 1, c + 2, lv(l0), :]),
                            (12, mm[c + 2]),
                        ][: 3 if k == 1 else 2]
                    if c == far:
                        pu = v[4] - v[2] if side == 0 else v[4] + v[2]
                        out = [(8, v[0]), (9, v[1]), (10, pu), (11, q)]
                    for n, value in out:
                        hs[k, side, n, lv(l0), :] = value.astype(BF16)
            return _

        over_chunks(body, 0)

    def send_halo(k):
        size = NHALO if k == 1 else NHALO - 1
        copies = [
            remote(hs.at[k, 0, :size], hr.at[k, 1, :size], left),
            remote(hs.at[k, 1, :size], hr.at[k, 0, :size], right),
        ]
        for copy in copies:
            copy.start()
        return copies

    for name in ("inc1", "traj", "land", "damp"):
        loads[name].wait()
    constants()
    prepare(1)
    n_edge = jnp.where(first, 0, 1) + jnp.where(last, 0, 1)
    pl.semaphore_wait(barrier, len(everyone) + n_edge)
    halo1 = send_halo(1)

    for name in ("inc0", "mul0", "mis0"):
        loads[name].wait()
    residual(0, True)
    b_copy = Shift(b_send, b_recv, -1)
    b_copy.start()

    @pl.when(last)
    def _():
        b_recv[...] = jnp.zeros_like(b_recv)

    @pl.when(first)
    def _():
        f_recv[...] = jnp.zeros_like(f_recv)

    prepare(0)
    halo0 = send_halo(0)

    subcount, nobs = cell_v.shape
    rows = ft.shape[1]
    block = 256
    columns = 8 * sp_n
    offset = sp * 8
    row_id = lax.broadcasted_iota(jnp.int32, (rows, block), 0)
    lane_id = lax.broadcasted_iota(jnp.int32, (LANES, block), 0)

    def sensors(k, total, lo, hi):
        if lo == 0:
            sensors_begin(k)
        total = lax.fori_loop(lo, hi, functools.partial(sensor_block, k), total)
        if hi == nobs // block:
            both = acc2[:, :LANES] + acc2[:, LANES:]
            spread[k] = both.reshape(spread.shape[1:])
        return total

    def sensors_begin(k):
        turned = inc_n[k * 5 : k * 5 + 2].reshape(rows, LANES).T
        high = turned.astype(BF16)
        ft[0:LANES, :] = high
        ft[LANES:, :] = (turned - high.astype(F32)).astype(BF16)
        acc2[...] = jnp.zeros_like(acc2)

    def sensor_block(k, n, total):
        at = pl.ds(pl.multiple_of(n * block, block), block)
        cell = cell_v[k : k + 1, at]
        row = cell & (LANES - 1)
        rest = cell >> 7
        col = rest & (columns - 1)
        level = rest >> (columns.bit_length() - 1)
        own = (col >= offset) & (col < offset + 8)
        local = jnp.where(own, level * 8 + col - offset, -1)
        hot = jnp.where(row_id == local, 1.0, 0.0).astype(BF16)
        on_lane = lane_id == row
        picked = jnp.dot(ft[...], hot, preferred_element_type=F32)
        both = picked[:LANES] + picked[LANES:]
        obs = jnp.sum(jnp.where(on_lane, both, 0.0), axis=0, keepdims=True)
        smul = smul_v[k : k + 1, at]
        res = inno_v[k : k + 1, at] - serr_v[k : k + 1, at] * smul - obs
        put = jnp.where(on_lane, smul + 0.5 * res, 0.0)
        put_high = put.astype(BF16)
        put_low = (put - put_high.astype(F32)).astype(BF16)
        put2 = jnp.concatenate([put_high, put_low], axis=0)
        acc2[...] += lax.dot_general(
            hot, put2, (((1,), (1,)), ((), ())), preferred_element_type=F32
        )
        so[0, k : k + 1, at] = obs
        return total + jnp.where(own, res * res, 0.0)

    for name in ("cell", "inno", "serr", "smul", "mul1", "mis1"):
        loads[name].wait()
    residual(1, False)
    blocks = nobs // block
    total = sensors(1, jnp.zeros((1, block), F32), 0, blocks // 2)
    b_copy.hand_on()
    total = sensors(1, total, blocks // 2, blocks)

    slot = [0]

    def obs_stage(stage, peers):
        copies = []
        for peer in peers:
            copies.append((remote(so.at[stage], so_recv.at[slot[0]], peer), slot[0]))
            copies[-1][0].start()
            slot[0] += 1
        return copies

    def obs_sum(stage, copies):
        value = so[stage]
        for copy, n in copies:
            copy.wait()
            value = value + so_recv[n]
        return value

    def unpack(k, copies):
        for copy in copies:
            copy.wait()

        def body(l0, _):
            for side, near, far in ((0, 1, 0), (1, 10, 11)):

                def got(n):
                    return hr[k, side, n, lv(l0), :].astype(F32)

                for f in range(5):
                    x[k, f, near, lv(l0), :] = got(f)
                q0[k, near, lv(l0), :] = got(5)
                kt[k, 1, near, lv(l0), :] = got(6)
                ks[k, 1, near, lv(l0), :] = got(7)
                if k == 1:
                    mm[near] = got(12)
                x[k, 0, far, lv(l0), :] = got(8)
                x[k, 1, far, lv(l0), :] = got(9)
                x[k, 2, far, lv(l0), :] = zero
                x[k, 4, far, lv(l0), :] = got(10)
                q0[k, far, lv(l0), :] = got(11)
            return _

        over_chunks(body, 0)

    def tangent(s, q, k, i, l0, m):
        def at(f, n):
            return s[k, f, n, lv(l0), :]

        t, sa, u, v, p = [at(f, i) for f in range(5)]
        qc = q[k, i, lv(l0), :]
        t2 = 0.4 * t + 0.15 * (at(0, i - 1) + at(0, i + 1)) + dn(t) + up(t)
        s2 = 0.4 * sa + 0.15 * (at(1, i - 1) + at(1, i + 1)) + dn(sa) + up(sa)
        u2 = u + r3 * v - 0.15 * (q[k, i + 1, lv(l0), :] - q[k, i - 1, lv(l0), :])
        v2 = v - r3 * u + dn(qc) - up(qc)
        east = at(4, i + 1) - at(2, i + 1)
        west = at(4, i - 1) + at(2, i - 1)
        p2 = 0.4 * p + 0.15 * (east + west) + up(p - v) + dn(p + v)
        return [m * w for w in (t2, s2, u2, v2, p2)]

    def first_substep(k):
        def body(l0, _):
            for i in range(1, 11):
                new = tangent(x, q0, k, i, l0, mm[i])
                for f in range(5):
                    y[k, f, i - 1, lv(l0), :] = new[f]
                q1[k, i - 1, lv(l0), :] = (
                    new[4] + kt[k, 1, i, lv(l0), :] * new[0] + ks[k, 1, i, lv(l0), :] * new[1]
                )
            return _

        over_chunks(body, 0)

    def second_substep(k):
        def body(l0, acc):
            for i in range(1, 9):
                c = i - 1
                m = mm[c + 2]
                new = tangent(y, q1, k, i, l0, m)
                for f in range(5):
                    if k == 1:
                        fw[f, c, lv(l0), :] = new[f]
                        f_send[f, c, lv(l0), :] = new[f].astype(BF16)
                    else:
                        r = r0[1, f, c, lv(l0), :] + new[f]
                        acc = acc + r * r
                        mn = mul_n[5 + f, nat(l0, c), :] + 0.5 * r
                        mn_n[5 + f, nat(l0, c), :] = mn
                        put_edge(0, f, c, l0, m * mn)
            return acc

        macc[...] = over_chunks(body, macc[...])

    def put_edge(k, f, c, l0, w):
        wa[k, f, c + 2, lv(l0), :] = w
        for side, near, far in ((0, 0, 1), (1, 7, 6)):
            if c == near:
                es[k, side, f, lv(l0), :] = w.astype(BF16)
            if c == far and f != 3:
                es[k, side, 5 + (f if f < 3 else 3), lv(l0), :] = w.astype(BF16)

    unpack(1, halo1)
    first_substep(1)
    second_substep(1)
    f_copy = Shift(f_send, f_recv, 1)
    f_copy.start()

    total = sensors(0, total, 0, blocks // 2)
    f_copy.hand_on()
    total = sensors(0, total, blocks // 2, blocks)
    unpack(0, halo0)
    first_substep(0)
    second_substep(0)

    def send_edges(k):
        copies = [
            remote(es.at[k, 0], er.at[k, 1], left),
            remote(es.at[k, 1], er.at[k, 0], right),
        ]
        for copy in copies:
            copy.start()
        return copies

    edges0 = send_edges(0)
    outs = []

    def store(src, dst, n):
        copy = pltpu.make_async_copy(src, dst, out_sem.at[n])
        copy.start()
        outs.append(copy)


    b_copy.wait_recv()

    keep = jnp.where(last, 0.0, 1.0)

    def following(l0, _):
        for c in range(8):
            m = keep * mm[c + 2]
            for f in range(5):
                u = b_recv[f, c, lv(l0), :].astype(F32) + 0.5 * fw[f, c, lv(l0), :]
                put_edge(1, f, c, l0, m * u)
        return _

    over_chunks(following, 0)
    edges1 = send_edges(1)

    def transposed(s, k, j, i, col, l0):
        def at(f, n):
            return s[k, f, n, lv(l0), :]

        t, sa, u, v, p = [at(f, i) for f in range(5)]
        pw, pe = at(4, i - 1), at(4, i + 1)
        q = 0.15 * (at(2, i + 1) - at(2, i - 1)) + up(v) - dn(v)
        t2 = 0.4 * t + 0.15 * (at(0, i - 1) + at(0, i + 1)) + dn(t) + up(t)
        t2 = t2 + kt[k, j, col, lv(l0), :] * q
        s2 = 0.4 * sa + 0.15 * (at(1, i - 1) + at(1, i + 1)) + dn(sa) + up(sa)
        s2 = s2 + ks[k, j, col, lv(l0), :] * q
        south, north = dn(p), up(p)
        u2 = u - r3 * v + 0.15 * (pe - pw)
        v2 = v + r3 * u + north - south
        p2 = 0.4 * p + 0.15 * (pe + pw) + south + north + q
        return [t2, s2, u2, v2, p2]

    def first_transposed(k):
        def body(l0, _):
            for i in range(1, 11):
                new = transposed(wa, k, 1, i, i, l0)
                m = mm[i]
                for f in range(5):
                    wb[k, f, i - 1, lv(l0), :] = m * new[f]
            return _

        over_chunks(body, 0)

    def second_transposed(k):
        def body(l0, acc):
            for i in range(1, 9):
                c = i - 1
                new = transposed(wb, k, 0, i, c + 2, l0)
                for f in range(5):
                    if k == 0:
                        rt[f, c, lv(l0), :] = new[f]
                    else:
                        g = mn_n[5 + f, nat(l0, c), :] - new[f]
                        if f < 2:
                            g = g + spread[1, f, nat(l0, c), :]
                        g_n[5 + f, nat(l0, c), :] = g
                        acc = acc + g * g
            return acc

        gacc[...] = over_chunks(body, gacc[...])

    def unpack_edges(k, copies):
        for copy in copies:
            copy.wait()

        def body(l0, _):
            for side, near, far in ((0, 1, 0), (1, 10, 11)):
                for n in range(NEDGE):
                    f = n if n < 5 else (0, 1, 2, 4)[n - 5]
                    i = near if n < 5 else far
                    wa[k, f, i, lv(l0), :] = er[k, side, n, lv(l0), :].astype(F32)
            return _

        over_chunks(body, 0)

    unpack_edges(0, edges0)
    first_transposed(0)
    second_transposed(0)

    unpack_edges(1, edges1)
    first_transposed(1)
    second_transposed(1)

    obs_copies = obs_stage(0, obs_y)
    f_copy.wait_recv()

    def finish(l0, carry):
        ma, ga = carry
        for f in range(5):
            for c in range(8):
                r = r0[0, f, c, lv(l0), :] + f_recv[f, c, lv(l0), :].astype(F32)
                ma = ma + r * r
                mn = mul_n[f, nat(l0, c), :] + 0.5 * r
                mn_n[f, nat(l0, c), :] = mn
                g = mn - rt[f, c, lv(l0), :]
                if f < 2:
                    g = g + spread[0, f, nat(l0, c), :]
                g_n[f, nat(l0, c), :] = g
                ga = ga + g * g
        return ma, ga

    ma, ga = over_chunks(finish, (macc[...], gacc[...]))
    ma = jnp.sum(ma, axis=0, keepdims=True) + total[:, :LANES] + total[:, LANES:]
    ga = jnp.sum(ga, axis=0, keepdims=True)
    sub = lax.broadcasted_iota(jnp.int32, (8, LANES), 0)
    value = jnp.where(sub == 0, ma, jnp.where(sub == 1, ga, 0.0))

    pending = []
    n = 0
    for stage, peers in enumerate((group_a, group_b, group_c)):
        ar[stage] = value
        copies = []
        for peer in peers:
            copies.append((remote(ar.at[stage], ar_recv.at[n], peer), n))
            copies[-1][0].start()
            n += 1
        for copy, m in copies:
            copy.wait_recv()
            value = value + ar_recv[m]
        pending += [copy for copy, _ in copies]
        observed = obs_sum(stage, obs_copies)
        if stage < 2:
            so[stage + 1] = observed
            obs_copies = obs_stage(stage + 1, (obs_y, obs_z, obs_c)[stage + 1])
    smul = smul_v[...]
    sens_n[...] = smul + 0.5 * (inno_v[...] - serr_v[...] * smul - observed)
    top = jnp.sum(value[0:1], axis=1, keepdims=True)
    below = jnp.sum(value[1:2], axis=1, keepdims=True)
    stride = jnp.broadcast_to(top / (below + 1e-6), (8, LANES))

    pieces = 5
    size = inc_n.shape[0] // pieces

    def update(n, _):
        for r in range(levels):
            at = pl.ds(r * 8, 8)
            inc_out[n, at, :] = inc_n[n, at, :] - stride * g_n[n, at, :]
        return _

    for n in range(pieces):
        at = pl.ds(n * size, size)
        lax.fori_loop(n * size, (n + 1) * size, update, 0)

    for copy in pending:
        copy.wait_send()

    b_copy.wait_send()
    f_copy.wait_send()

    for copy in outs:
        copy.wait()


def on_device(
    dims,
    increment,
    multiplier,
    sensor_multiplier,
    misfit,
    innovation,
    model_error,
    sensor_error,
    trajectory,
    land_sea,
    sensor_cells,
):
    subcount, fields, levels, width, latitude = increment.shape
    rows = levels * width
    nobs = sensor_cells.shape[1]
    zh_n, x_n, y_n, zl_n, c_n = dims
    flat = (subcount * fields, rows, latitude)
    vm = pl.BlockSpec(memory_space=pltpu.VMEM)
    hbm = pl.BlockSpec(memory_space=pltpu.HBM)
    n_obs = (y_n - 1) + (zl_n - 1) + (c_n - 1)
    n_ar = (y_n * c_n - 1) + (x_n - 1) + (zh_n * zl_n - 1)
    n_sem = 10 + 6 * NRELAY + n_obs + n_ar

    def v(*shape, dtype=F32):
        return pltpu.VMEM(shape, dtype)

    lr = (levels, latitude)
    increment_next, mult_next, sensor_next = pl.pallas_call(
        functools.partial(main_kernel, dims),
        out_shape=(
            jax.ShapeDtypeStruct(flat, F32),
            jax.ShapeDtypeStruct(flat, F32),
            jax.ShapeDtypeStruct((subcount, nobs), F32),
        ),
        in_specs=[hbm] * 10,
        out_specs=(vm, vm, vm),
        scratch_shapes=[
            v(*flat), v(*flat), v(*flat),
            v(subcount, 2, 2, rows, latitude, dtype=BF16),
            v(*flat),
            v(width, latitude, dtype=jnp.int32), v(fields, levels),
            v(subcount, nobs, dtype=jnp.int32),
            v(subcount, nobs), v(subcount, nobs), v(subcount, nobs),
            v(fields, *lr),
            v(subcount, 2, rows, latitude),
            v(2 * LANES, 2 * rows, dtype=BF16),
            v(2 * rows, 2 * LANES),
            v(subcount, fields, 12, *lr),
            v(subcount, 2, 12, *lr), v(subcount, 2, 12, *lr),
            v(subcount, 12, *lr),
            v(subcount, fields, 10, *lr),
            v(subcount, 10, *lr),
            v(fields, 8, *lr),
            v(subcount, fields, 8, *lr),
            v(subcount, fields, 12, *lr),
            v(subcount, fields, 10, *lr),
            v(fields, 8, *lr),
            v(12, CH, latitude),
            v(2, 8 * CH, latitude),
            v(subcount, 2, NHALO, *lr, dtype=BF16),
            v(subcount, 2, NHALO, *lr, dtype=BF16),
            v(subcount, 2, NEDGE, *lr, dtype=BF16),
            v(subcount, 2, NEDGE, *lr, dtype=BF16),
            v(fields, 8, *lr, dtype=BF16), v(fields, 8, *lr, dtype=BF16),
            v(fields, 8, *lr, dtype=BF16), v(fields, 8, *lr, dtype=BF16),
            v(NRELAY, 8, *lr, dtype=BF16),
            v(CH, latitude), v(CH, latitude),
            v(3, subcount, nobs), v(n_obs, subcount, nobs),
            v(3, 8, latitude), v(n_ar, 8, latitude),
            pltpu.SemaphoreType.DMA((13,)),
            pltpu.SemaphoreType.DMA((n_sem,)),
            pltpu.SemaphoreType.DMA((n_sem,)),
        ],
        compiler_params=pltpu.CompilerParams(
            vmem_limit_bytes=46 << 20, collective_id=0, has_side_effects=True
        ),
        name="uzawa",
    )(*[pltpu.with_memory_space_constraint(a, pltpu.HBM) for a in (
        increment.reshape(flat),
        multiplier.reshape(flat),
        misfit.reshape(flat),
        trajectory.reshape(subcount, 2, 2, rows, latitude),
        land_sea,
        model_error,
        sensor_cells,
        innovation,
        sensor_error,
        sensor_multiplier,
    )])
    return (
        increment_next.reshape(increment.shape),
        mult_next.reshape(increment.shape),
        sensor_next,
    )


def solution(mesh, dims=DIMS):
    return jax.shard_map(
        functools.partial(on_device, dims),
        mesh=mesh,
        in_specs=(
            P("tm", None, None, "space", None),
            P("tm", None, None, "space", None),
            P("tm", None),
            P("tm", None, None, "space", None),
            P("tm", None),
            P(),
            P("tm", None),
            P("tm", None, None, None, "space", None),
            P("space", None),
            P("tm", None),
        ),
        out_specs=(
            P("tm", None, None, "space", None),
            P("tm", None, None, "space", None),
            P("tm", None),
        ),
        check_vma=False,
    )
```
